256 devices in a mesh: section: 2 (over y_hi), seq: 16 (over z, y_lo), tp: 8 (over x, core).
Axes of the slice: x: 4, y: 4 (y_hi: 2, y_lo: 2; y = y_hi * 2 + y_lo), z: 8, core: 2. Of those that a mesh axis runs over, the one named last changes fastest.
Arguments:
- layer_input: bfloat16 [2, 4096, 4096], P('section', 'seq'), may hold values from -500 to 500
- upstream: bfloat16 [2, 4096, 4096], P('section', 'seq'), may hold values from -6 to 6
- norm_gain: bfloat16 [2, 4096], P('section'), may hold values from 0.5 to 1.5
- query_weight: bfloat16 [2, 4096, 2048], P('section', 'seq', 'tp'), may hold values from -0.0625 to 0.0625
- key_weight: bfloat16 [2, 4096, 1024], P('section', 'seq', 'tp'), may hold values from -0.0625 to 0.0625
- value_weight: bfloat16 [2, 4096, 1024], P('section', 'seq', 'tp'), may hold values from -0.09375 to 0.09375
- output_weight: bfloat16 [2, 4096, 2048], P('section', 'seq', 'tp'), may hold values from -0.125 to 0.125
Outputs:
- passed_grad: bfloat16 [2, 4096, 4096], P('section', 'seq')
- query_grad: bfloat16 [2, 4096, 2048], P('section', 'seq', 'tp')
- key_grad: bfloat16 [2, 4096, 1024], P('section', 'seq', 'tp')
- value_grad: bfloat16 [2, 4096, 1024], P('section', 'seq', 'tp')
- output_grad: bfloat16 [2, 4096, 2048], P('section', 'seq', 'tp')
- gain_grad: float32 [2, 4096], P('section', 'tp')
The draws below stay inside these ranges and needn't reach their ends.
All inputs are finite; a program needn't handle non-finite values.
Results may differ from the reference program's by a relative error of at most 0.023.
Values may be sent and summed in bfloat16 or wider, within the bound.
A program may use at most 64 MiB of HBM per device.

```python
import math
import jax
import jax.numpy as jnp
from jax import lax

D = 4096
HEADS = 16
KV_HEADS = 8
HEAD_DIM = 128
WINDOW = 2048
BLOCK = 256
TOKENS = 4096
N_SEQ = 16
N_TP = 8


def projection_pair(base_key):
    fan_scale = 1.0 / math.sqrt(D)
    query_part = jnp.clip(jax.random.normal(jax.random.fold_in(base_key, 101), (2, D, HEADS * HEAD_DIM), jnp.float32), -4.0, 4.0) * fan_scale
    key_part = jnp.clip(jax.random.normal(jax.random.fold_in(base_key, 102), (2, D, KV_HEADS * HEAD_DIM), jnp.float32), -4.0, 4.0) * fan_scale
    return (query_part, key_part)


def draw_query_weight(key, part):
    return projection_pair(key)[0].astype(jnp.bfloat16)


def draw_key_weight(key, part):
    return projection_pair(key)[1].astype(jnp.bfloat16)


def draw_layer_input(key, part):
    noise_field = jnp.clip(jax.random.normal(jax.random.fold_in(key, 103), (2, TOKENS, D), jnp.float32), -6.0, 6.0)
    return noise_field.astype(jnp.bfloat16)


def steps_of(own_key, dims, pieces, smallest, top_value):
    level = 1.0
    for axis_at, blocks in pieces:
        draws = jax.random.uniform(jax.random.fold_in(jax.random.fold_in(own_key, 6), axis_at), (blocks,), jnp.float32, smallest / len(pieces), top_value / len(pieces))
        level = level * jnp.repeat(jnp.exp(draws), dims[axis_at] // blocks).reshape((-1,) + (1,) * (len(dims) - 1 - axis_at))
    return level


def noise(rng, extent, deviation, bound, split=(), kind=jnp.bfloat16):
    loudness = steps_of(rng, extent, split, -0.22, 0.18) if split else 1.0
    drawn = jax.random.normal(rng, extent, jnp.float32) * deviation * loudness
    return jnp.minimum(jnp.maximum(drawn, -bound), bound).astype(kind)


def setup_inputs(seed: int = 0) -> dict:
    key_of = jax.random.split(jax.random.key(seed), 8)
    return {
        "layer_input": draw_layer_input(jax.random.fold_in(key_of[7], 71), 0),
        "upstream": noise(key_of[1], (2, TOKENS, D), 1.0, 6.0, ((0, 2), (1, 16))),
        "norm_gain": jnp.clip(1.0 + 0.1 * jax.random.normal(key_of[2], (2, D), jnp.float32), 0.5, 1.5).astype(jnp.bfloat16),
        "query_weight": draw_query_weight(jax.random.fold_in(key_of[7], 71), 0),
        "key_weight": draw_key_weight(jax.random.fold_in(key_of[7], 71), 0),
        "value_weight": noise(key_of[5], (2, D, KV_HEADS * HEAD_DIM), D ** -0.5, 0.09375, ((0, 2), (1, 16), (2, 8))),
        "output_weight": noise(key_of[6], (2, D, HEADS * HEAD_DIM), (HEADS * HEAD_DIM) ** -0.5, 0.125, ((0, 2), (1, 16), (2, 8))),
    }


epsilon = 1e-05

def rotate(values, positions, direction_sign):
    half_width = values.shape[-1] // 2
    frequency = jnp.exp(jnp.arange(half_width, dtype=jnp.float32) * (-2.0 * math.log(10000.0) / values.shape[-1]))
    angles = positions[:, None] * frequency[None, :]
    cosine = jnp.cos(angles)[:, None, :]
    sine_table = direction_sign * jnp.sin(angles)[:, None, :]
    first_half = values[..., :half_width]
    second_half = values[..., half_width:]
    return jnp.concatenate([first_half * cosine - second_half * sine_table, second_half * cosine + first_half * sine_table], axis=-1)

def layer_backward(layer_input, upstream, norm_gain, query_weight, key_weight, value_weight, output_weight):
    tokens_all = layer_input.shape[0]
    input_values = layer_input.astype(jnp.float32)
    inverse_norm = lax.rsqrt(lax.optimization_barrier(jnp.mean(input_values * input_values, axis=-1, keepdims=True)) + epsilon)
    gain_values = norm_gain.astype(jnp.float32)
    normed = (input_values * inverse_norm * gain_values).astype(jnp.bfloat16)
    positions = jnp.arange(tokens_all).astype(jnp.float32)
    query_vectors = rotate(jnp.dot(normed, query_weight, preferred_element_type=jnp.float32).reshape(tokens_all, HEADS, HEAD_DIM), positions, 1.0).astype(jnp.bfloat16)
    key_vectors = rotate(jnp.dot(normed, key_weight, preferred_element_type=jnp.float32).reshape(tokens_all, KV_HEADS, HEAD_DIM), positions, 1.0).astype(jnp.bfloat16)
    value_vectors = jnp.dot(normed, value_weight, preferred_element_type=jnp.float32).astype(jnp.bfloat16).reshape(tokens_all, KV_HEADS, HEAD_DIM)
    attn_delta = jnp.dot(upstream, output_weight, preferred_element_type=jnp.float32).astype(jnp.bfloat16).reshape(tokens_all, HEADS, HEAD_DIM)
    group_size = HEADS // KV_HEADS
    score_scale = 1.0 / math.sqrt(HEAD_DIM)
    halo_blocks = min((WINDOW + BLOCK - 2) // BLOCK, N_SEQ - 1)
    span_rows = (halo_blocks + 1) * BLOCK
    pad_rows = halo_blocks * BLOCK
    padding = jnp.zeros((pad_rows, KV_HEADS, HEAD_DIM), jnp.bfloat16)
    keys_padded = jnp.concatenate([padding, key_vectors], axis=0)
    values_padded = jnp.concatenate([padding, value_vectors], axis=0)

    def attend(carry, block_index):
        key_total, value_total = carry
        first_row = (block_index * BLOCK).astype(jnp.int32)
        query_block = lax.dynamic_slice_in_dim(query_vectors, first_row, BLOCK, 0).astype(jnp.float32)
        delta_block = lax.dynamic_slice_in_dim(attn_delta, first_row, BLOCK, 0).astype(jnp.float32)
        key_slab = lax.dynamic_slice_in_dim(keys_padded, first_row, span_rows, 0).astype(jnp.float32)
        value_slab = lax.dynamic_slice_in_dim(values_padded, first_row, span_rows, 0).astype(jnp.float32)
        key_heads = jnp.repeat(key_slab, group_size, axis=1)
        value_heads = jnp.repeat(value_slab, group_size, axis=1)
        query_position = first_row + jnp.arange(BLOCK).astype(jnp.int32)
        key_position = first_row - pad_rows + jnp.arange(span_rows).astype(jnp.int32)
        allowed = (key_position[None, :] <= query_position[:, None]) & (key_position[None, :] > query_position[:, None] - WINDOW) & (key_position[None, :] >= 0)
        scores = jnp.einsum('thd,uhd->htu', query_block, key_heads) * score_scale
        scores = jnp.where(allowed[None], scores, -1e+30)
        row_peak = lax.optimization_barrier(jnp.max(scores, axis=-1, keepdims=True))
        exponent_terms = jnp.exp(scores - row_peak)
        softmax_probs = exponent_terms / lax.optimization_barrier(jnp.sum(exponent_terms, axis=-1, keepdims=True))
        rounded_probs = softmax_probs.astype(jnp.bfloat16).astype(jnp.float32)
        attended = jnp.einsum('htu,uhd->thd', rounded_probs, value_heads).astype(jnp.bfloat16)
        softmax_delta = jnp.einsum('thd,uhd->htu', delta_block, value_heads)
        row_delta = lax.optimization_barrier(jnp.sum(delta_block * attended.astype(jnp.float32), axis=-1))
        score_delta = (softmax_probs * (softmax_delta - jnp.transpose(row_delta)[:, :, None]) * score_scale).astype(jnp.bfloat16).astype(jnp.float32)
        query_rot_delta = jnp.einsum('htu,uhd->thd', score_delta, key_heads)
        key_part = jnp.einsum('htu,thd->uhd', score_delta, query_block).reshape(span_rows, KV_HEADS, group_size, HEAD_DIM).sum(axis=2)
        value_part = jnp.einsum('htu,thd->uhd', rounded_probs, delta_block).reshape(span_rows, KV_HEADS, group_size, HEAD_DIM).sum(axis=2)
        key_total = lax.dynamic_update_slice_in_dim(key_total, lax.dynamic_slice_in_dim(key_total, first_row, span_rows, 0) + key_part, first_row, 0)
        value_total = lax.dynamic_update_slice_in_dim(value_total, lax.dynamic_slice_in_dim(value_total, first_row, span_rows, 0) + value_part, first_row, 0)
        return ((key_total, value_total), (attended, query_rot_delta))
    start_carry = (jnp.zeros((pad_rows + tokens_all, KV_HEADS, HEAD_DIM), jnp.float32), jnp.zeros((pad_rows + tokens_all, KV_HEADS, HEAD_DIM), jnp.float32))
    (key_total, value_total), (attended, query_rot_delta) = lax.scan(attend, start_carry, jnp.arange(N_SEQ).astype(jnp.int32))
    attended = attended.reshape(tokens_all, HEADS * HEAD_DIM)
    query_rot_delta = query_rot_delta.reshape(tokens_all, HEADS, HEAD_DIM)
    query_delta = rotate(query_rot_delta, positions, -1.0).astype(jnp.bfloat16).reshape(tokens_all, HEADS * HEAD_DIM)
    key_delta = rotate(key_total[pad_rows:], positions, -1.0).astype(jnp.bfloat16).reshape(tokens_all, KV_HEADS * HEAD_DIM)
    value_delta = value_total[pad_rows:].astype(jnp.bfloat16).reshape(tokens_all, KV_HEADS * HEAD_DIM)
    head_share = HEADS // N_TP * HEAD_DIM
    kv_share = KV_HEADS // N_TP * HEAD_DIM
    normed_delta = jnp.zeros((tokens_all, D), jnp.float32)
    for group_index in range(N_TP):
        query_cols = slice(group_index * head_share, (group_index + 1) * head_share)
        kv_cols = slice(group_index * kv_share, (group_index + 1) * kv_share)
        partial_value = jnp.dot(query_delta[:, query_cols], query_weight[:, query_cols].T, preferred_element_type=jnp.float32)
        partial_value = partial_value + jnp.dot(key_delta[:, kv_cols], key_weight[:, kv_cols].T, preferred_element_type=jnp.float32)
        partial_value = partial_value + jnp.dot(value_delta[:, kv_cols], value_weight[:, kv_cols].T, preferred_element_type=jnp.float32)
        normed_delta = normed_delta + lax.optimization_barrier(partial_value.astype(jnp.bfloat16)).astype(jnp.float32)
    row_dot = lax.optimization_barrier(jnp.sum(gain_values * normed_delta * input_values, axis=-1, keepdims=True))
    input_delta = (upstream.astype(jnp.float32) + inverse_norm * gain_values * normed_delta - input_values * inverse_norm * inverse_norm * inverse_norm * row_dot / D).astype(jnp.bfloat16)
    gain_grad = lax.optimization_barrier(jnp.sum(normed_delta * input_values * inverse_norm, axis=0))
    deltas_all = jnp.concatenate([query_delta, key_delta, value_delta], axis=1)

    def seq_partial(totals, block_index):
        first_row = (block_index * BLOCK).astype(jnp.int32)
        normed_rows = lax.dynamic_slice_in_dim(normed, first_row, BLOCK, 0)
        delta_rows = lax.dynamic_slice_in_dim(deltas_all, first_row, BLOCK, 0)
        upstream_rows = lax.dynamic_slice_in_dim(upstream, first_row, BLOCK, 0)
        attended_rows = lax.dynamic_slice_in_dim(attended, first_row, BLOCK, 0)
        part_in = jnp.dot(normed_rows.T, delta_rows, preferred_element_type=jnp.float32)
        part_out = jnp.dot(upstream_rows.T, attended_rows, preferred_element_type=jnp.float32)
        part_in = lax.optimization_barrier(part_in.astype(jnp.bfloat16)).astype(jnp.float32)
        part_out = lax.optimization_barrier(part_out.astype(jnp.bfloat16)).astype(jnp.float32)
        return ((totals[0] + part_in, totals[1] + part_out), None)
    zero_in = jnp.zeros((D, (HEADS + 2 * KV_HEADS) * HEAD_DIM), jnp.float32)
    zero_out = jnp.zeros((D, HEADS * HEAD_DIM), jnp.float32)
    (grads_in, grads_out), unused = lax.scan(seq_partial, (zero_in, zero_out), jnp.arange(N_SEQ).astype(jnp.int32))
    query_grad = grads_in[:, :HEADS * HEAD_DIM].astype(jnp.bfloat16)
    key_grad = grads_in[:, HEADS * HEAD_DIM:(HEADS + KV_HEADS) * HEAD_DIM].astype(jnp.bfloat16)
    value_grad = grads_in[:, (HEADS + KV_HEADS) * HEAD_DIM:].astype(jnp.bfloat16)
    output_grad = grads_out.astype(jnp.bfloat16)
    return (input_delta, query_grad, key_grad, value_grad, output_grad, gain_grad)

def reference(layer_input, upstream, norm_gain, query_weight, key_weight, value_weight, output_weight):
    results = []
    for section_index in range(2):
        results.append(layer_backward(layer_input[section_index], upstream[section_index], norm_gain[section_index], query_weight[section_index], key_weight[section_index], value_weight[section_index], output_weight[section_index]))
    passed_grad = jnp.stack([results[1][0], results[0][0]], axis=0)
    query_grad = jnp.stack([results[0][1], results[1][1]], axis=0)
    key_grad = jnp.stack([results[0][2], results[1][2]], axis=0)
    value_grad = jnp.stack([results[0][3], results[1][3]], axis=0)
    output_grad = jnp.stack([results[0][4], results[1][4]], axis=0)
    gain_grad = jnp.stack([results[0][5], results[1][5]], axis=0)
    return (passed_grad, query_grad, key_grad, value_grad, output_grad, gain_grad)
```

```python
import math

import jax
import jax.numpy as jnp
import numpy as np
from jax import lax
from jax.experimental import pallas as pl
from jax.experimental.pallas import tpu as pltpu
from jax.sharding import Mesh
from jax.sharding import PartitionSpec as P

AXES = ("section", "z", "y", "x", "c")
MESH = pl.DeviceIdType.MESH
D = 4096
HD = 128
WINDOW = 2048
B = 256
NZ = 8
NX = 4
EPS = 1e-05
SCALE = 1.0 / math.sqrt(HD)
F32 = jnp.float32
BF = jnp.bfloat16
RIGHT = (4, 4, 3)
LEFT = (3, 3, 4)


def nt(a, b):
    return lax.dot_general(a, b, (((1,), (1,)), ((), ())), preferred_element_type=F32)


def nn(a, b):
    return lax.dot_general(a, b, (((1,), (0,)), ((), ())), preferred_element_type=F32)


def kernel(
    x_hbm, u_hbm, qw, kw, vw, ow, gain, off_c, off_s, blk_c, blk_s,
    og, gq, gk, gv, go, gg,
    wbuf, xs, xr, xin, invb, isend, irecv, acc, pbuf, rbuf, cosb, sinb,
    qb, kv, dob, qt, dot_, sb, db, mb, lb, oacc, dqa, delta,
    dkve, ysrc, yrcv, zsrc, zrcv, dl, dlt, rds, rdr, rdx, rdy, rdb,
    gs, gr, npo, cs, cr, rss, rsr, nd, ps, gb, gyr,
    l_w, l_x, l_u, l_r,
    w_s, w_r, x_s, x_r, i_s, i_r, p_s, p_r,
    kz_s, ky_s, kv_r, yr_s, yr_r, zr_s, zr_r, d_s, d_r,
    rd_s, rd_r, g_s, g_r, c_s, c_r, n_s, n_r, ps_s, ps_r,
    og_s, og_r, gb_s, gb_r, gy_s, gy_r,
):
    sec = lax.axis_index("section")
    z = lax.axis_index("z")
    y = lax.axis_index("y")
    x = lax.axis_index("x")
    c = lax.axis_index("c")
    s = 2 * z + y
    t = 2 * x + c
    zr_, zl_ = lax.rem(z + 1, NZ), lax.rem(z + NZ - 1, NZ)
    xp, xm, xa = lax.rem(x + 1, NX), lax.rem(x + NX - 1, NX), lax.rem(x + 2, NX)
    py, pc, psec = 1 - y, 1 - c, 1 - sec
    to_y = {"y": py}
    to_c = {"c": pc}
    own = pl.ds(pl.multiple_of(y * B, B), B)
    oth = pl.ds(pl.multiple_of(py * B, B), B)

    def rc(src, dst, ss, rs, dev):
        return pltpu.make_async_remote_copy(
            src_ref=src, dst_ref=dst, send_sem=ss, recv_sem=rs,
            device_id=dev, device_id_type=MESH,
        )

    sends = []

    def send(src, dst, ss, rs, dev):
        copy = rc(src, dst, ss, rs, dev)
        copy.start()
        sends.append(copy)
        return copy

    def arrived(dst, ss, rs, dev):
        rc(dst, dst, ss, rs, dev).wait_recv()

    loads = [
        pltpu.make_async_copy(kw, wbuf.at[z, 0, :, pl.ds(0, HD)], l_w.at[0]),
        pltpu.make_async_copy(vw, wbuf.at[z, 0, :, pl.ds(HD, HD)], l_w.at[1]),
        pltpu.make_async_copy(qw, wbuf.at[z, 1], l_w.at[2]),
        pltpu.make_async_copy(ow, wbuf.at[z, 2], l_w.at[3]),
        pltpu.make_async_copy(x_hbm, xin, l_x),
    ]
    for copy in loads:
        copy.start()

    def cols(blk, parity):
        return pl.ds(pl.multiple_of((2 * blk + parity) * B, B), B)

    for j in range(NZ):
        pltpu.make_async_copy(u_hbm.at[:, cols(j, y)], xs.at[1, j, own, :], l_u).start()
        pltpu.make_async_copy(x_hbm.at[:, cols(j, y)], xr.at[j, own, :], l_r).start()

    barrier = pltpu.get_barrier_semaphore()
    greet = [
        {"z": zr_}, {"z": zl_}, to_y, to_c, {"x": xp}, {"x": xm}, {"x": xa},
        {"section": psec}, {"section": psec, "y": py},
    ]
    for dev in greet:
        pl.semaphore_signal(barrier, inc=1, device_id=dev, device_id_type=MESH)
    pl.semaphore_wait(barrier, len(greet))

    for copy in loads[:4]:
        copy.wait()

    def w_send(h, ch):
        if h < RIGHT[ch]:
            blk = lax.rem(z + NZ - h, NZ)
            send(wbuf.at[blk, ch], wbuf.at[blk, ch], w_s.at[0, h, ch], w_r.at[0, h, ch], {"z": zr_})
        if h < LEFT[ch]:
            blk = lax.rem(z + h, NZ)
            send(wbuf.at[blk, ch], wbuf.at[blk, ch], w_s.at[1, h, ch], w_r.at[1, h, ch], {"z": zl_})

    def w_wait(h, ch):
        if h <= RIGHT[ch]:
            blk = lax.rem(z + NZ - h, NZ)
            arrived(wbuf.at[blk, ch], w_s.at[0, h - 1, ch], w_r.at[0, h - 1, ch], {"z": zr_})
        if h <= LEFT[ch]:
            blk = lax.rem(z + h, NZ)
            arrived(wbuf.at[blk, ch], w_s.at[1, h - 1, ch], w_r.at[1, h - 1, ch], {"z": zl_})

    for ch in range(3):
        w_send(0, ch)

    mine = pl.ds(pl.multiple_of(c * 128, 128), 128)
    there = pl.ds(pl.multiple_of(y * B + c * 128, 128), 128)
    from_y = pl.ds(pl.multiple_of(py * B + c * 128, 128), 128)
    from_c = pl.ds(pl.multiple_of(py * B + pc * 128, 128), 128)
    for j in range(NZ):
        rc(x_hbm.at[mine, cols(j, py)], xr.at[j, there, :], x_s.at[0], x_r.at[0], to_y).start()
    for j in range(NZ):
        rc(u_hbm.at[mine, cols(j, py)], xs.at[1, j, there, :], x_s.at[1], x_r.at[1], to_y).start()
    x_out = rc(xr.at[:, from_y, :], xr.at[:, there, :], x_s.at[0], x_r.at[0], to_y)
    u_out = rc(xs.at[1, :, from_y, :], xs.at[1, :, there, :], x_s.at[1], x_r.at[1], to_y)

    lane = lax.broadcasted_iota(jnp.int32, (B, HD), 1)
    cosb[...] = blk_c[s] * off_c[...] - blk_s[s] * off_s[...]
    sin_all = blk_s[s] * off_c[...] + blk_c[s] * off_s[...]
    sinb[...] = jnp.where(lane < HD // 2, -sin_all, sin_all)

    loads[4].wait()
    invb[own, :] = jnp.zeros((B, HD), F32)

    def squares(j, _):
        v = xin[:, pl.ds(pl.multiple_of(j * B, B), B)].astype(F32)
        invb[own, :] += v[:, :HD] * v[:, :HD] + v[:, HD:] * v[:, HD:]
        return 0

    lax.fori_loop(0, D // B, squares, 0)
    mean = jnp.sum(invb[own, :], axis=1, keepdims=True) / D
    inv_own = jnp.broadcast_to(lax.rsqrt(mean + EPS), (B, HD))
    invb[own, :] = inv_own
    isend[...] = jnp.transpose(inv_own)[:8, :]
    send(isend, irecv, i_s, i_r, to_y)

    whole = pltpu.make_async_copy(xs.at[1, :, oth, :], xs.at[1, :, own, :], l_u)
    whole.wait()
    pltpu.make_async_copy(xr.at[:, oth, :], xr.at[:, own, :], l_r).wait()

    def norm_rows(rows):
        def step(j, _):
            inv = invb[rows, :]
            g = gain[2 * j + y]
            v = xr[j, rows, :].astype(F32)
            n = jnp.concatenate([v[:, :HD] * inv, v[:, HD:] * inv], axis=1) * g
            xs[0, j, rows, :] = n.astype(BF)
            return 0

        lax.fori_loop(0, NZ, step, 0)

    norm_rows(own)

    for h in (1, 2, 3):
        for ch in range(3):
            w_wait(h, ch)
            w_send(h, ch)
        if h == 2:
            x_out.wait_recv()
            send(xr.at[:, from_y, :], xr.at[:, from_y, :], x_s.at[2], x_r.at[2], to_c)
            u_out.wait_recv()
            send(xs.at[1, :, from_y, :], xs.at[1, :, from_y, :], x_s.at[3], x_r.at[3], to_c)

    arrived(irecv, i_s, i_r, to_y)
    inv_oth = jnp.transpose(jnp.broadcast_to(irecv[0:1, :], (HD, B)))
    invb[oth, :] = inv_oth
    arrived(xr.at[:, from_c, :], x_s.at[2], x_r.at[2], to_c)
    norm_rows(oth)
    arrived(xs.at[1, :, from_c, :], x_s.at[3], x_r.at[3], to_c)

    acc[...] = jnp.zeros_like(acc)

    def project(blk, ch):
        sel = jnp.where(ch == 2, 1, 0)
        acc[ch] += nn(xs[sel, blk], wbuf[blk, ch])

    def project_most(n, _):
        project(lax.rem(z + 5 + lax.div(n, 3), NZ), lax.rem(n, 3))
        return 0

    lax.fori_loop(0, 21, project_most, 0)
    for ch in range(3):
        w_wait(4, ch)

    def project_last(ch, _):
        project(lax.rem(z + 4, NZ), ch)
        pbuf[ch] = acc[ch, oth, :].astype(BF)
        rc(pbuf.at[ch], rbuf.at[ch], p_s.at[ch], p_r.at[ch], to_y).start()
        return 0

    lax.fori_loop(0, 3, project_last, 0)
    for ch in range(3):
        sends.append(rc(pbuf.at[ch], rbuf.at[ch], p_s.at[ch], p_r.at[ch], to_y))

    def total(ch):
        arrived(rbuf.at[ch], p_s.at[ch], p_r.at[ch], to_y)
        return acc[ch, own, :] + rbuf[ch].astype(F32)

    def rot(v, sign):
        return v * cosb[...] + pltpu.roll(v, HD // 2, 1) * (sign * sinb[...])

    both = total(0)
    kv[0, 0] = rot(both[:, :HD], 1.0).astype(BF)
    kv[0, 1] = both[:, HD:].astype(BF)

    def kz_send(i, k):
        send(kv.at[2 * i, k], kv.at[2 * i + 2, k], kz_s.at[i, k], kv_r.at[2 * i + 2, k], {"z": zr_})

    def ky_copy(i, k):
        return rc(kv.at[2 * i + 2 * y, k], kv.at[2 * i + 1, k], ky_s.at[i, k], kv_r.at[2 * i + 1, k], to_y)

    for k in range(2):
        kz_send(0, k)

    @pl.when(y == 0)
    def _():
        for k in range(2):
            ky_copy(0, k).start()

    both = total(1)
    for h in range(2):
        q = rot(both[:, h * HD : (h + 1) * HD], 1.0)
        qb[h] = q.astype(BF)
        qt[h] = jnp.transpose(q).astype(BF)
    both = total(2)
    for h in range(2):
        v = both[:, h * HD : (h + 1) * HD]
        dob[h] = v.astype(BF)
        dot_[h] = jnp.transpose(v).astype(BF)

    mb[...] = jnp.full(mb.shape, -3e38, F32)
    diff = lax.broadcasted_iota(jnp.int32, (B, B), 1) - lax.broadcasted_iota(jnp.int32, (B, B), 0)

    def scores(d, _):
        top = jnp.where(s >= d, d * B, -2 * WINDOW)
        allowed = (diff <= top) & (diff > d * B - WINDOW)
        for h in range(2):
            sc = jnp.where(allowed, nt(qb[h], kv[d, 0]) * SCALE, -1e30)
            sb[h, d] = sc
            mb[h] = jnp.maximum(mb[h], jnp.maximum(sc[:, :HD], sc[:, HD:]))
            db[h, d] = nt(dob[h], kv[d, 1])
        return 0

    for i in range(4):
        for k in range(2):
            arrived(kv.at[2 * i + 2, k], kz_s.at[i, k], kv_r.at[2 * i + 2, k], {"z": zr_})
            if i < 3:
                kz_send(i + 1, k)

                @pl.when(y == 0)
                def _():
                    ky_copy(i + 1, k).start()

            @pl.when(y == 1)
            def _():
                ky_copy(i, k).start()

    for i in range(4):
        for k in range(2):
            arrived(kv.at[2 * i + 1, k], ky_s.at[i, k], kv_r.at[2 * i + 1, k], to_y)
            sends.append(ky_copy(i, k))
    lax.fori_loop(0, 9, scores, 0)

    for h in range(2):
        m = jnp.broadcast_to(jnp.max(mb[h], axis=1, keepdims=True), (B, HD))
        mb[h] = m
        lb[h] = jnp.zeros((B, HD), F32)

    def exps(d, _):
        for h in range(2):
            m = mb[h]
            e = jnp.exp(sb[h, d] - jnp.concatenate([m, m], axis=1))
            sb[h, d] = e
            lb[h] += e[:, :HD] + e[:, HD:]
        return 0

    lax.fori_loop(0, 9, exps, 0)
    for h in range(2):
        lb[h] = jnp.broadcast_to(1.0 / jnp.sum(lb[h], axis=1, keepdims=True), (B, HD))
        oacc[h] = jnp.zeros((B, HD), F32)
        dqa[h] = jnp.zeros((B, HD), F32)

    def attend(d, _):
        for h in range(2):
            l = lb[h]
            p = sb[h, d] * jnp.concatenate([l, l], axis=1)
            sb[h, d] = p
            oacc[h] += nn(p.astype(BF), kv[d, 1])
        return 0

    lax.fori_loop(0, 9, attend, 0)
    for h in range(2):
        att = oacc[h].astype(BF)
        dl[2, own, pl.ds(h * HD, HD)] = att
        delta[h] = jnp.broadcast_to(
            jnp.sum(att.astype(F32) * dob[h].astype(F32), axis=1, keepdims=True), (B, HD)
        )

    def dl_send(ch):
        send(dl.at[ch, own, :], dl.at[ch, own, :], d_s.at[ch], d_r.at[ch], to_y)

    dl_send(2)

    def slot_grads(d):
        dkt = jnp.zeros((HD, B), F32)
        dvt = jnp.zeros((HD, B), F32)
        for h in range(2):
            p = sb[h, d]
            r = delta[h]
            ds = (p * (db[h, d] - jnp.concatenate([r, r], axis=1)) * SCALE).astype(BF)
            dqa[h] += nn(ds, kv[d, 0])
            dkt = dkt + nn(qt[h], ds)
            dvt = dvt + nn(dot_[h], p.astype(BF))
        return dkt, dvt

    def y_copy(i):
        return rc(ysrc.at[i], yrcv.at[i], yr_s.at[i], yr_r.at[i], to_y)

    def backward(i, _):
        @pl.when(i < 4)
        def _():
            a, b = slot_grads(7 - 2 * i)
            ysrc[3 - i, 0] = a.astype(BF)
            ysrc[3 - i, 1] = b.astype(BF)
            y_copy(3 - i).start()

        a, b = slot_grads(8 - 2 * i)
        dkve[4 - i, 0] = a
        dkve[4 - i, 1] = b
        return 0

    lax.fori_loop(0, 5, backward, 0)

    for h in range(2):
        dl[1, own, pl.ds(h * HD, HD)] = rot(dqa[h], -1.0).astype(BF)
    dl_send(1)

    def from_partner(e):
        i = e // 2 - y
        keep = jnp.where((i >= 0) & (i < 4), 1.0, 0.0)
        return yrcv[jnp.clip(i, 0, 3)].astype(F32) * keep

    for i in range(4):
        e = 8 - 2 * i
        y_copy(3 - i).wait_recv()
        sends.append(y_copy(3 - i))
        part = dkve[e // 2] + from_partner(e)
        if i > 0:
            arrived(zrcv.at[i - 1], zr_s.at[i - 1], zr_r.at[i - 1], {"z": zl_})
            part = part + zrcv[i - 1].astype(F32)
        zsrc[i] = part.astype(BF)
        send(zsrc.at[i], zrcv.at[i], zr_s.at[i], zr_r.at[i], {"z": zl_})
    arrived(zrcv.at[3], zr_s.at[3], zr_r.at[3], {"z": zl_})
    part = dkve[0] + from_partner(0) + zrcv[3].astype(F32)
    dk = jnp.transpose(part[0])
    dv = jnp.transpose(part[1])
    dl[0, own, pl.ds(0, HD)] = rot(dk, -1.0).astype(BF)
    dl[0, own, pl.ds(HD, HD)] = dv.astype(BF)
    dl_send(0)

    rd = dk * kv[0, 0].astype(F32) + dv * kv[0, 1].astype(F32)
    for h in range(2):
        rd = rd + dqa[h] * qb[h].astype(F32)
    rd = jnp.broadcast_to(jnp.sum(rd, axis=1, keepdims=True), (B, HD))
    rds[0] = jnp.transpose(rd)[:8, :]
    send(rds.at[0], rdr, rd_s.at[0], rd_r.at[0], to_c)

    def dlt_make(ch):
        arrived(dl.at[ch, oth, :], d_s.at[ch], d_r.at[ch], to_y)
        dlt[ch] = jnp.transpose(dl[ch].astype(F32)).astype(BF)

    for ch in range(3):
        dlt_make(ch)

    def parts(i, pc_):
        b = 2 * i + pc_
        return nt(dl[0], wbuf[b, 0]) + nt(dl[1], wbuf[b, 1])

    def parts_out(i, _):
        cs[i] = parts(i, pc).astype(BF)
        rc(cs.at[i], cr.at[i], c_s.at[i], c_r.at[i], to_c).start()
        return 0

    lax.fori_loop(0, NX, parts_out, 0)
    for i in range(NX):
        sends.append(rc(cs.at[i], cr.at[i], c_s.at[i], c_r.at[i], to_c))

    def parts_own(i, _):
        npo[i] = parts(i, c)
        return 0

    lax.fori_loop(0, NX, parts_own, 0)

    def g_copy(way, j, ch):
        dev = {"z": jnp.where(way == 0, zr_, zl_)}
        return rc(gs.at[way, j, ch], gr.at[way, j, ch], g_s.at[way, j, ch], g_r.at[way, j, ch], dev)

    def weight_part(blk, ch):
        sel = jnp.where(ch == 2, 1, 0)
        return nn(dlt[ch], xs[sel, blk])

    def w_step(j):
        count = 6 if j < 3 else 3

        def one(n, _):
            if j < 3:
                ch, way = 2 - lax.div(n, 2), lax.rem(n, 2)
                length = jnp.where((ch < 2) == (way == 0), 4, 3)
            else:
                ch = 2 - n
                way = jnp.where(ch < 2, 0, 1)
                length = 4
            step = jnp.where(way == 0, length - j, NZ - (length - j))
            part = weight_part(lax.rem(z + step, NZ), ch)
            if j > 0:
                g_copy(way, j - 1, ch).wait_recv()
                part = part + gr[way, j - 1, ch].astype(F32)
            gs[way, j, ch] = part.astype(BF)
            g_copy(way, j, ch).start()
            return 0

        lax.fori_loop(0, count, one, 0)

    w_step(0)

    for i in range(NX):
        arrived(cr.at[i], c_s.at[i], c_r.at[i], to_c)
    npo[...] += cr[...].astype(F32)
    up, low = pl.ds(0, B), pl.ds(B, B)

    def r_send(way, k):
        dev = {"x": xp} if way == 0 else {"x": xm}
        send(rss.at[way, k], rsr.at[way, k], n_s.at[way, k], n_r.at[way, k], dev)

    def r_wait(way, k):
        arrived(rsr.at[way, k], n_s.at[way, k], n_r.at[way, k], {"x": xp})

    rss[0, 0] = npo[xa, up, :].astype(BF)
    rss[1, 0] = npo[xa, low, :].astype(BF)
    r_send(0, 0)
    r_send(1, 0)
    rss[0, 1] = npo[xp, low, :].astype(BF)
    rss[1, 1] = npo[xm, up, :].astype(BF)
    r_send(0, 1)
    r_send(1, 1)

    arrived(rdr, rd_s.at[0], rd_r.at[0], to_c)
    rds[1] = rds[0] + rdr[...]
    for k, dev in enumerate(({"x": xp}, {"x": xm}, {"x": xa})):
        send(rds.at[1], rdx.at[k], rd_s.at[1 + k], rd_r.at[1 + k], dev)

    r_wait(0, 0)
    rss[0, 2] = (npo[xp, up, :] + rsr[0, 0].astype(F32)).astype(BF)
    r_send(0, 2)
    r_wait(1, 0)
    rss[1, 2] = (npo[xm, low, :] + rsr[1, 0].astype(F32)).astype(BF)
    r_send(1, 2)

    w_step(1)

    for k in range(3):
        arrived(rdx.at[k], rd_s.at[1 + k], rd_r.at[1 + k], {"x": xp})
    rds[2] = rds[1] + rdx[0] + rdx[1] + rdx[2]
    send(rds.at[2], rdy, rd_s.at[4], rd_r.at[4], to_y)
    rdb[own, :] = jnp.transpose(jnp.broadcast_to(rds[2, 0:1, :], (HD, B)))

    r_wait(0, 1)
    r_wait(1, 1)
    r_wait(0, 2)
    r_wait(1, 2)
    nd[up, :] = npo[x, up, :] + rsr[0, 2].astype(F32) + rsr[1, 1].astype(F32)
    nd[low, :] = npo[x, low, :] + rsr[0, 1].astype(F32) + rsr[1, 2].astype(F32)
    arrived(rdy, rd_s.at[4], rd_r.at[4], to_y)
    rdb[oth, :] = jnp.transpose(jnp.broadcast_to(rdy[0:1, :], (HD, B)))

    for hf in range(2):
        cut = pl.ds(hf * HD, HD)
        inv = invb[...]
        v = xr[t, :, cut].astype(F32)
        n = nd[:, cut]
        g = gain[2 * t + y, :, cut]
        out = xs[1, t, :, cut].astype(F32) + inv * g * n - v * (inv * inv) * rdb[...] * (1.0 / D)
        ps[:, cut] = out.astype(BF)
        gpart = jnp.sum(n * v * inv, axis=0, keepdims=True)
        gb[z, :, cut] = jnp.broadcast_to(gpart, (8, HD))
    send(ps.at[own, :], og.at[t, y], ps_s.at[0], ps_r.at[0], {"section": psec})
    send(ps.at[oth, :], og.at[t, y], ps_s.at[1], ps_r.at[1], {"section": psec, "y": py})

    def gb_send(h):
        blk = lax.rem(z + NZ - h, NZ)
        send(gb.at[blk], gb.at[blk], gb_s.at[0, h], gb_r.at[0, h], {"z": zr_})
        if h < 3:
            blk = lax.rem(z + h, NZ)
            send(gb.at[blk], gb.at[blk], gb_s.at[1, h], gb_r.at[1, h], {"z": zl_})

    def gb_wait(h):
        blk = lax.rem(z + NZ - h, NZ)
        arrived(gb.at[blk], gb_s.at[0, h - 1], gb_r.at[0, h - 1], {"z": zr_})
        if h < 4:
            blk = lax.rem(z + h, NZ)
            arrived(gb.at[blk], gb_s.at[1, h - 1], gb_r.at[1, h - 1], {"z": zl_})

    gb_send(0)

    w_step(2)

    gb_wait(1)
    gb_send(1)

    arrived(og.at[t, y], ps_s.at[0], ps_r.at[0], {"section": psec})
    arrived(og.at[t, py], ps_s.at[1], ps_r.at[1], {"section": psec, "y": py})
    tr, tl, ta = 2 * xm + c, 2 * xp + c, 2 * xa + c

    def og_send(blk, lo, n, k, dev):
        send(og.at[blk, pl.ds(lo, n)], og.at[blk, pl.ds(lo, n)], og_s.at[k], og_r.at[k], dev)

    def og_wait(blk, lo, n, k):
        arrived(og.at[blk, pl.ds(lo, n)], og_s.at[k], og_r.at[k], to_c)

    og_send(t, 0, 1, 0, {"x": xp})
    og_send(t, 1, 1, 1, {"x": xm})
    og_send(t, 1, 1, 2, {"x": xp})
    og_send(t, 0, 1, 3, {"x": xm})
    og_send(t, 0, 2, 4, to_c)

    w_step(3)

    gb_wait(2)
    gb_send(2)

    og_wait(tr, 0, 1, 0)
    og_send(tr, 0, 1, 5, {"x": xp})
    og_wait(tl, 1, 1, 1)
    og_send(tl, 1, 1, 6, {"x": xm})
    og_wait(tr, 1, 1, 2)
    og_send(tr, 0, 2, 7, to_c)
    og_wait(tl, 0, 1, 3)
    og_send(tl, 0, 2, 8, to_c)

    gb_wait(3)
    gb_send(3)

    for ch in (2, 1, 0):
        part = weight_part(z, ch)
        for way, last in ((0, RIGHT[ch] - 1), (1, LEFT[ch] - 1)):
            g_copy(way, last, ch).wait_recv()
            part = part + gr[way, last, ch].astype(F32)
        part = jnp.transpose(part).astype(BF)
        if ch == 2:
            go[...] = part
        elif ch == 1:
            gq[...] = part
        else:
            gk[...] = part[:, :HD]
            gv[...] = part[:, HD:]
    for ch in range(3):
        for j in range(RIGHT[ch]):
            sends.append(g_copy(0, j, ch))
        for j in range(LEFT[ch]):
            sends.append(g_copy(1, j, ch))

    og_wait(ta, 0, 1, 5)
    og_send(ta, 0, 1, 9, to_c)
    og_wait(ta, 1, 1, 6)
    og_send(ta, 1, 1, 10, to_c)

    gb_wait(4)
    gsum = gb[0]
    for i in range(1, NZ):
        gsum = gsum + gb[i]
    gg[y] = gsum
    send(gg.at[y], gg.at[y], gy_s, gy_r, to_y)

    sib = 1 - 2 * c
    og_wait(t + sib, 0, 2, 4)
    og_wait(tr + sib, 0, 2, 7)
    og_wait(tl + sib, 0, 2, 8)
    og_wait(ta + sib, 0, 1, 9)
    og_wait(ta + sib, 1, 1, 10)
    arrived(gg.at[py], gy_s, gy_r, to_y)
    for copy in sends:
        copy.wait_send()
    x_out.wait_send()
    u_out.wait_send()


def tables():
    freq = 10000.0 ** (-2.0 * np.arange(HD // 2) / HD)
    freq = np.concatenate([freq, freq])
    off = np.arange(B)[:, None] * freq[None, :]
    blk = (np.arange(16) * B)[:, None, None] * freq[None, None, :]
    return [a.astype(np.float32) for a in (np.cos(off), np.sin(off), np.cos(blk), np.sin(blk))]


def per_device(layer_input, upstream, norm_gain, query_weight, key_weight, value_weight, output_weight):
    gain = norm_gain[0].astype(F32).reshape(16, 1, B)
    dma = pltpu.SemaphoreType.DMA
    vm = pltpu.VMEM
    scratch = [
        vm((NZ, 3, B, B), BF), vm((2, NZ, 2 * B, B), BF), vm((NZ, 2 * B, B), BF), vm((B, D), BF),
        vm((2 * B, HD), F32), vm((8, B), F32), vm((8, B), F32), vm((3, 2 * B, B), F32),
        vm((3, B, B), BF), vm((3, B, B), BF), vm((B, HD), F32), vm((B, HD), F32),
        vm((2, B, HD), BF), vm((9, 2, B, HD), BF), vm((2, B, HD), BF), vm((2, HD, B), BF), vm((2, HD, B), BF),
        vm((2, 9, B, B), F32), vm((2, 9, B, B), F32),
        vm((2, B, HD), F32), vm((2, B, HD), F32), vm((2, B, HD), F32), vm((2, B, HD), F32), vm((2, B, HD), F32),
        vm((5, 2, HD, B), F32), vm((4, 2, HD, B), BF), vm((4, 2, HD, B), BF), vm((4, 2, HD, B), BF), vm((4, 2, HD, B), BF),
        vm((3, 2 * B, B), BF), vm((3, B, 2 * B), BF),
        vm((3, 8, B), F32), vm((8, B), F32), vm((3, 8, B), F32), vm((8, B), F32), vm((2 * B, HD), F32),
        vm((2, 4, 3, B, B), BF), vm((2, 4, 3, B, B), BF),
        vm((NX, 2 * B, B), F32), vm((NX, 2 * B, B), BF), vm((NX, 2 * B, B), BF),
        vm((2, 3, B, B), BF), vm((2, 3, B, B), BF), vm((2 * B, B), F32), vm((2 * B, B), BF),
        vm((NZ, 8, B), F32), vm((8, B), F32),
        dma((4,)), dma, dma, dma,
        dma((2, 4, 3)), dma((2, 4, 3)), dma((4,)), dma((4,)), dma, dma, dma((3,)), dma((3,)),
        dma((4, 2)), dma((4, 2)), dma((9, 2)), dma((4,)), dma((4,)), dma((4,)), dma((4,)), dma((3,)), dma((3,)),
        dma((5,)), dma((5,)), dma((2, 4, 3)), dma((2, 4, 3)), dma((4,)), dma((4,)), dma((2, 3)), dma((2, 3)),
        dma((2,)), dma((2,)),
        dma((11,)), dma((11,)), dma((2, 4)), dma((2, 4)), dma, dma,
    ]
    hbm = pl.BlockSpec(memory_space=pl.ANY)
    vmem = pl.BlockSpec(memory_space=pltpu.VMEM)
    og, gq, gk, gv, go, gg = pl.pallas_call(
        kernel,
        out_shape=[
            jax.ShapeDtypeStruct((8, 2, B, B), BF),
            jax.ShapeDtypeStruct((B, B), BF),
            jax.ShapeDtypeStruct((B, HD), BF),
            jax.ShapeDtypeStruct((B, HD), BF),
            jax.ShapeDtypeStruct((B, B), BF),
            jax.ShapeDtypeStruct((2, 8, B), F32),
        ],
        in_specs=[hbm] * 6 + [vmem] * 5,
        out_specs=[vmem] * 6,
        scratch_shapes=scratch,
        compiler_params=pltpu.CompilerParams(
            collective_id=0, has_side_effects=True, vmem_limit_bytes=60 * 1024 * 1024
        ),
        name="step",
    )(
        layer_input[0], upstream[0], query_weight[0], key_weight[0], value_weight[0], output_weight[0],
        gain, *tables(),
    )
    passed = jnp.transpose(og, (2, 0, 1, 3)).reshape(1, B, D)
    return passed, gq[None], gk[None], gv[None], go[None], gg[:, 0, :].reshape(1, 2 * B)


def solution(mesh):
    split = Mesh(mesh.devices.reshape(2, NZ, 2, NX, 2), AXES)
    seq, tp = ("z", "y"), ("x", "c")
    rows = P("section", seq, None)
    weight = P("section", seq, tp)
    return jax.shard_map(
        per_device,
        mesh=split,
        in_specs=(rows, rows, P("section", None), weight, weight, weight, weight),
        out_specs=(rows, weight, weight, weight, weight, P("section", tp)),
        check_vma=False,
    )
```

```python
import math

import jax
import jax.numpy as jnp
import numpy as np
from jax import lax
from jax.experimental import pallas as pl
from jax.experimental.pallas import tpu as pltpu
from jax.sharding import Mesh
from jax.sharding import PartitionSpec as P

AXES = ("section", "z", "y", "x", "c")
MESH = pl.DeviceIdType.MESH
D = 4096
HD = 128
WINDOW = 2048
B = 256
NZ = 8
NX = 4
EPS = 1e-05
SCALE = 1.0 / math.sqrt(HD)
F32 = jnp.float32
BF = jnp.bfloat16
RIGHT = (4, 4, 3)
LEFT = (3, 3, 4)


def nt(a, b):
    return lax.dot_general(a, b, (((1,), (1,)), ((), ())), preferred_element_type=F32)


def nn(a, b):
    return lax.dot_general(a, b, (((1,), (0,)), ((), ())), preferred_element_type=F32)


def kernel(
    x_hbm, u_hbm, qw, kw, vw, ow, gain, off_c, off_s, blk_c, blk_s,
    og, gq, gk, gv, go, gg,
    gainf, rel, wbuf, xs, xr, xin, invb, isend, irecv, acc, pbuf, rbuf, cosb, sinb,
    qb, kv, dob, qt, dot_, sb, db, mb, lb, oacc, dqa, delta,
    dkve, ysrc, yrcv, zsrc, zrcv, dl, dlt, rds, rdr, rdx, rdy, rdb,
    gs, gr, npart, cs, cr, rss, rsr, nd, ps, gb,
    l_w, l_x, l_u, l_r,
    w_s, w_r, x_s, x_r, i_s, i_r, p_s, p_r,
    kz_s, ky_s, kv_r, yr_s, yr_r, zr_s, zr_r, d_s, d_r,
    rd_s, rd_r, g_s, g_r, c_s, c_r, n_s, n_r, ps_s, ps_r,
    og_s, og_r, gb_s, gb_r, gy_s, gy_r,
):
    sec = lax.axis_index("section")
    z = lax.axis_index("z")
    y = lax.axis_index("y")
    x = lax.axis_index("x")
    c = lax.axis_index("c")
    s = 2 * z + y
    t = 2 * x + c
    zr_, zl_ = lax.rem(z + 1, NZ), lax.rem(z + NZ - 1, NZ)
    xp, xm, xa = lax.rem(x + 1, NX), lax.rem(x + NX - 1, NX), lax.rem(x + 2, NX)
    py, pc, psec = 1 - y, 1 - c, 1 - sec
    to_y = {"y": py}
    to_c = {"c": pc}
    own = pl.ds(pl.multiple_of(y * B, B), B)
    oth = pl.ds(pl.multiple_of(py * B, B), B)

    def rc(src, dst, ss, rs, dev):
        return pltpu.make_async_remote_copy(
            src_ref=src, dst_ref=dst, send_sem=ss, recv_sem=rs,
            device_id=dev, device_id_type=MESH,
        )

    sends = []

    def send(src, dst, ss, rs, dev):
        copy = rc(src, dst, ss, rs, dev)
        copy.start()
        sends.append(copy)
        return copy

    def arrived(dst, ss, rs, dev):
        rc(dst, dst, ss, rs, dev).wait_recv()

    loads = [
        pltpu.make_async_copy(kw, wbuf.at[z, 0, :, pl.ds(0, HD)], l_w.at[0]),
        pltpu.make_async_copy(vw, wbuf.at[z, 0, :, pl.ds(HD, HD)], l_w.at[1]),
        pltpu.make_async_copy(qw, wbuf.at[z, 1], l_w.at[2]),
        pltpu.make_async_copy(ow, wbuf.at[z, 2], l_w.at[3]),
        pltpu.make_async_copy(x_hbm, xin, l_x),
    ]
    for copy in loads:
        copy.start()

    def cols(blk, parity):
        return pl.ds(pl.multiple_of((2 * blk + parity) * B, B), B)

    for j in range(NZ):
        pltpu.make_async_copy(u_hbm.at[:, cols(j, y)], xs.at[1, j, own, :], l_u).start()
        pltpu.make_async_copy(x_hbm.at[:, cols(j, y)], xr.at[j, own, :], l_r).start()

    barrier = pltpu.get_barrier_semaphore()
    greet = [
        {"z": zr_}, {"z": zl_}, to_y, to_c, {"x": xp}, {"x": xm}, {"x": xa},
        {"section": psec, "y": py},
    ]
    for dev in greet:
        pl.semaphore_signal(barrier, inc=1, device_id=dev, device_id_type=MESH)
    pl.semaphore_wait(barrier, len(greet))

    for copy in loads[:4]:
        copy.wait()

    def w_send(h, ch):
        if h < RIGHT[ch]:
            blk = lax.rem(z + NZ - h, NZ)
            send(wbuf.at[blk, ch], wbuf.at[blk, ch], w_s.at[0, h, ch], w_r.at[0, h, ch], {"z": zr_})
        if h < LEFT[ch]:
            blk = lax.rem(z + h, NZ)
            send(wbuf.at[blk, ch], wbuf.at[blk, ch], w_s.at[1, h, ch], w_r.at[1, h, ch], {"z": zl_})

    def w_wait(h, ch):
        if h <= RIGHT[ch]:
            blk = lax.rem(z + NZ - h, NZ)
            arrived(wbuf.at[blk, ch], w_s.at[0, h - 1, ch], w_r.at[0, h - 1, ch], {"z": zr_})
        if h <= LEFT[ch]:
            blk = lax.rem(z + h, NZ)
            arrived(wbuf.at[blk, ch], w_s.at[1, h - 1, ch], w_r.at[1, h - 1, ch], {"z": zl_})

    for ch in range(3):
        w_send(0, ch)

    mine = pl.ds(pl.multiple_of(c * 128, 128), 128)
    there = pl.ds(pl.multiple_of(y * B + c * 128, 128), 128)
    from_y = pl.ds(pl.multiple_of(py * B + c * 128, 128), 128)
    from_c = pl.ds(pl.multiple_of(py * B + pc * 128, 128), 128)
    for j in range(NZ):
        rc(x_hbm.at[mine, cols(j, py)], xr.at[j, there, :], x_s.at[0], x_r.at[0], to_y).start()
    for j in range(NZ):
        rc(u_hbm.at[mine, cols(j, py)], xs.at[1, j, there, :], x_s.at[1], x_r.at[1], to_y).start()
    x_out = rc(xr.at[:, from_y, :], xr.at[:, there, :], x_s.at[0], x_r.at[0], to_y)
    u_out = rc(xs.at[1, :, from_y, :], xs.at[1, :, there, :], x_s.at[1], x_r.at[1], to_y)

    for j in range(D // B):
        gainf[j] = gain[:, j * B : (j + 1) * B].astype(F32)

    lane = lax.broadcasted_iota(jnp.int32, (B, HD), 1)
    cosb[...] = blk_c[s] * off_c[...] - blk_s[s] * off_s[...]
    sin_all = blk_s[s] * off_c[...] + blk_c[s] * off_s[...]
    sinb[...] = jnp.where(lane < HD // 2, -sin_all, sin_all)

    loads[4].wait()
    invb[own, :] = jnp.zeros((B, HD), F32)

    def squares(j, _):
        v = xin[:, pl.ds(pl.multiple_of(j * B, B), B)].astype(F32)
        invb[own, :] += v[:, :HD] * v[:, :HD] + v[:, HD:] * v[:, HD:]
        return 0

    lax.fori_loop(0, D // B, squares, 0)
    mean = jnp.sum(invb[own, :], axis=1, keepdims=True) / D
    inv_own = jnp.broadcast_to(lax.rsqrt(mean + EPS), (B, HD))
    invb[own, :] = inv_own
    isend[...] = jnp.transpose(inv_own)[:8, :]
    send(isend, irecv, i_s, i_r, to_y)

    whole = pltpu.make_async_copy(xs.at[1, :, oth, :], xs.at[1, :, own, :], l_u)
    whole.wait()
    pltpu.make_async_copy(xr.at[:, oth, :], xr.at[:, own, :], l_r).wait()

    def norm_rows(rows):
        def step(j, _):
            inv = invb[rows, :]
            g = gainf[2 * j + y]
            v = xr[j, rows, :].astype(F32)
            n = jnp.concatenate([v[:, :HD] * inv, v[:, HD:] * inv], axis=1) * g
            xs[0, j, rows, :] = n.astype(BF)
            return 0

        lax.fori_loop(0, NZ, step, 0)

    norm_rows(own)

    for h in (1, 2, 3):
        for ch in range(3):
            w_wait(h, ch)
            w_send(h, ch)
        if h == 2:
            x_out.wait_recv()
            send(xr.at[:, from_y, :], xr.at[:, from_y, :], x_s.at[2], x_r.at[2], to_c)
            u_out.wait_recv()
            send(xs.at[1, :, from_y, :], xs.at[1, :, from_y, :], x_s.at[3], x_r.at[3], to_c)

    arrived(irecv, i_s, i_r, to_y)
    inv_oth = jnp.transpose(jnp.broadcast_to(irecv[0:1, :], (HD, B)))
    invb[oth, :] = inv_oth
    arrived(xr.at[:, from_c, :], x_s.at[2], x_r.at[2], to_c)
    norm_rows(oth)
    arrived(xs.at[1, :, from_c, :], x_s.at[3], x_r.at[3], to_c)

    acc[...] = jnp.zeros_like(acc)

    def project(blk, ch):
        sel = jnp.where(ch == 2, 1, 0)
        acc[ch] += nn(xs[sel, blk], wbuf[blk, ch])

    def project_most(n, _):
        project(lax.rem(z + 5 + lax.div(n, 3), NZ), lax.rem(n, 3))
        return 0

    lax.fori_loop(0, 21, project_most, 0)
    for ch in range(3):
        w_wait(4, ch)

    def project_last(ch, _):
        project(lax.rem(z + 4, NZ), ch)
        pbuf[ch] = acc[ch, oth, :].astype(BF)
        rc(pbuf.at[ch], rbuf.at[ch], p_s.at[ch], p_r.at[ch], to_y).start()
        return 0

    lax.fori_loop(0, 3, project_last, 0)
    for ch in range(3):
        sends.append(rc(pbuf.at[ch], rbuf.at[ch], p_s.at[ch], p_r.at[ch], to_y))

    def total(ch):
        arrived(rbuf.at[ch], p_s.at[ch], p_r.at[ch], to_y)
        return acc[ch, own, :] + rbuf[ch].astype(F32)

    def rot(v, sign):
        return v * cosb[...] + pltpu.roll(v, HD // 2, 1) * (sign * sinb[...])

    both = total(0)
    kv[0, 0] = rot(both[:, :HD], 1.0).astype(BF)
    kv[0, 1] = both[:, HD:].astype(BF)

    def kz_send(i, k):
        send(kv.at[2 * i, k], kv.at[2 * i + 2, k], kz_s.at[i, k], kv_r.at[2 * i + 2, k], {"z": zr_})

    def ky_copy(i, k):
        return rc(kv.at[2 * i + 2 * y, k], kv.at[2 * i + 1, k], ky_s.at[i, k], kv_r.at[2 * i + 1, k], to_y)

    for k in range(2):
        kz_send(0, k)

    @pl.when(y == 0)
    def _():
        for k in range(2):
            ky_copy(0, k).start()

    both = total(1)
    for h in range(2):
        q = rot(both[:, h * HD : (h + 1) * HD], 1.0)
        qb[h] = q.astype(BF)
        qt[h] = jnp.transpose(q).astype(BF)
    both = total(2)
    for h in range(2):
        v = both[:, h * HD : (h + 1) * HD]
        dob[h] = v.astype(BF)
        dot_[h] = jnp.transpose(v).astype(BF)

    mb[...] = jnp.full(mb.shape, -3e38, F32)
    diff = lax.broadcasted_iota(jnp.int32, (B, B), 1) - lax.broadcasted_iota(jnp.int32, (B, B), 0)

    def scores(d, _):
        top = jnp.where(s >= d, d * B, -2 * WINDOW)
        allowed = (diff <= top) & (diff > d * B - WINDOW)
        for h in range(2):
            sc = jnp.where(allowed, nt(qb[h], kv[d, 0]) * SCALE, -1e30)
            sb[h, d] = sc
            mb[h] = jnp.maximum(mb[h], jnp.maximum(sc[:, :HD], sc[:, HD:]))
            db[h, d] = nt(dob[h], kv[d, 1])
        return 0

    for i in range(4):
        for k in range(2):
            arrived(kv.at[2 * i + 2, k], kz_s.at[i, k], kv_r.at[2 * i + 2, k], {"z": zr_})
            if i < 3:
                kz_send(i + 1, k)

                @pl.when(y == 0)
                def _():
                    ky_copy(i + 1, k).start()

            @pl.when(y == 1)
            def _():
                ky_copy(i, k).start()

    for i in range(4):
        for k in range(2):
            arrived(kv.at[2 * i + 1, k], ky_s.at[i, k], kv_r.at[2 * i + 1, k], to_y)
            sends.append(ky_copy(i, k))
    lax.fori_loop(0, 9, scores, 0)

    for h in range(2):
        m = jnp.broadcast_to(jnp.max(mb[h], axis=1, keepdims=True), (B, HD))
        mb[h] = m
        lb[h] = jnp.zeros((B, HD), F32)

    def exps(d, _):
        for h in range(2):
            m = mb[h]
            e = jnp.exp(sb[h, d] - jnp.concatenate([m, m], axis=1))
            sb[h, d] = e
            lb[h] += e[:, :HD] + e[:, HD:]
        return 0

    lax.fori_loop(0, 9, exps, 0)
    for h in range(2):
        lb[h] = jnp.broadcast_to(1.0 / jnp.sum(lb[h], axis=1, keepdims=True), (B, HD))
        oacc[h] = jnp.zeros((B, HD), F32)
        dqa[h] = jnp.zeros((B, HD), F32)

    def attend(d, _):
        for h in range(2):
            l = lb[h]
            p = sb[h, d] * jnp.concatenate([l, l], axis=1)
            sb[h, d] = p
            oacc[h] += nn(p.astype(BF), kv[d, 1])
        return 0

    lax.fori_loop(0, 9, attend, 0)
    for h in range(2):
        att = oacc[h].astype(BF)
        dl[2, own, pl.ds(h * HD, HD)] = att
        delta[h] = jnp.broadcast_to(
            jnp.sum(att.astype(F32) * dob[h].astype(F32), axis=1, keepdims=True), (B, HD)
        )

    def dl_send(ch):
        send(dl.at[ch, own, :], dl.at[ch, own, :], d_s.at[ch], d_r.at[ch], to_y)

    dl_send(2)

    def slot_grads(d):
        dkt = jnp.zeros((HD, B), F32)
        dvt = jnp.zeros((HD, B), F32)
        for h in range(2):
            p = sb[h, d]
            r = delta[h]
            ds = (p * (db[h, d] - jnp.concatenate([r, r], axis=1)) * SCALE).astype(BF)
            dqa[h] += nn(ds, kv[d, 0])
            dkt = dkt + nn(qt[h], ds)
            dvt = dvt + nn(dot_[h], p.astype(BF))
        return dkt, dvt

    def y_copy(i):
        return rc(ysrc.at[i], yrcv.at[i], yr_s.at[i], yr_r.at[i], to_y)

    def slot_pair(i):
        a, b = slot_grads(2 * i + 1)
        ysrc[i, 0] = a.astype(BF)
        ysrc[i, 1] = b.astype(BF)
        y_copy(i).start()
        sends.append(y_copy(i))
        a, b = slot_grads(2 * i + 2)
        dkve[i + 1, 0] = a
        dkve[i + 1, 1] = b

    def from_partner(e):
        i = e // 2 - y
        keep = jnp.where((i >= 0) & (i < 4), 1.0, 0.0)
        return yrcv[jnp.clip(i, 0, 3)].astype(F32) * keep

    def chain(i):
        e = 8 - 2 * i
        y_copy(3 - i).wait_recv()
        part = dkve[e // 2] + from_partner(e)
        if i > 0:
            arrived(zrcv.at[i - 1], zr_s.at[i - 1], zr_r.at[i - 1], {"z": zl_})
            part = part + zrcv[i - 1].astype(F32)
        zsrc[i] = part.astype(BF)
        send(zsrc.at[i], zrcv.at[i], zr_s.at[i], zr_r.at[i], {"z": zl_})

    def dlt_make(ch):
        dlt[ch] = jnp.transpose(dl[ch].astype(F32)).astype(BF)

    def g_copy(way, j, ch):
        dev = {"z": zr_ if way == 0 else zl_}
        return rc(gs.at[way, j, ch], gr.at[way, j, ch], g_s.at[way, j, ch], g_r.at[way, j, ch], dev)

    def weight_part(blk, ch):
        return nn(dlt[ch], xs[1 if ch == 2 else 0, blk])

    def g(way, j, ch):
        step = 4 - j if way == 0 else NZ - (3 - j)
        part = weight_part(lax.rem(z + step, NZ), ch)
        if j > 0:
            g_copy(way, j - 1, ch).wait_recv()
            part = part + gr[way, j - 1, ch].astype(F32)
        gs[way, j, ch] = part.astype(BF)
        copy = g_copy(way, j, ch)
        copy.start()
        sends.append(copy)

    slot_pair(3)
    slot_pair(2)
    chain(0)
    slot_pair(1)
    chain(1)
    slot_pair(0)
    a, b = slot_grads(0)
    dkve[0, 0] = a
    dkve[0, 1] = b
    for h in range(2):
        dl[1, own, pl.ds(h * HD, HD)] = rot(dqa[h], -1.0).astype(BF)
    dl_send(1)
    chain(2)
    arrived(dl.at[2, oth, :], d_s.at[2], d_r.at[2], to_y)
    dlt_make(2)
    g(0, 0, 2)
    chain(3)
    arrived(dl.at[1, oth, :], d_s.at[1], d_r.at[1], to_y)
    dlt_make(1)
    g(0, 0, 1)
    g(0, 1, 2)

    def query_parts(b, _):
        npart[b] = nt(dl[1], wbuf[b, 1])
        return 0

    lax.fori_loop(0, NZ, query_parts, 0)

    arrived(zrcv.at[3], zr_s.at[3], zr_r.at[3], {"z": zl_})
    part = dkve[0] + from_partner(0) + zrcv[3].astype(F32)
    dk = jnp.transpose(part[0])
    dv = jnp.transpose(part[1])
    dl[0, own, pl.ds(0, HD)] = rot(dk, -1.0).astype(BF)
    dl[0, own, pl.ds(HD, HD)] = dv.astype(BF)
    dl_send(0)

    rd = dk * kv[0, 0].astype(F32) + dv * kv[0, 1].astype(F32)
    for h in range(2):
        rd = rd + dqa[h] * qb[h].astype(F32)
    rd = jnp.broadcast_to(jnp.sum(rd, axis=1, keepdims=True), (B, HD))
    rds[0] = jnp.transpose(rd)[:8, :]
    send(rds.at[0], rdr, rd_s.at[0], rd_r.at[0], to_c)

    def c_copy(k, i, rows):
        return rc(cs.at[i, rows, :], cr.at[i, rows, :], c_s.at[k, i], c_r.at[k, i], to_c)

    def parts(k, rows):
        def out(i, _):
            b = 2 * i + pc
            cs[i, rows, :] = (npart[b, rows, :] + nt(dl[0, rows, :], wbuf[b, 0])).astype(BF)
            c_copy(k, i, rows).start()
            return 0

        def keep(i, _):
            b = 2 * i + c
            npart[b, rows, :] += nt(dl[0, rows, :], wbuf[b, 0])
            return 0

        lax.fori_loop(0, NX, out, 0)
        lax.fori_loop(0, NX, keep, 0)
        for i in range(NX):
            sends.append(c_copy(k, i, rows))

    def pair_sum(k, rows):
        for i in range(NX):
            c_copy(k, i, rows).wait_recv()

        def add(i, _):
            npart[2 * i + c, rows, :] += cr[i, rows, :].astype(F32)
            return 0

        lax.fori_loop(0, NX, add, 0)

    def r_send(way, k, blk, rows, add=None):
        part = npart[2 * blk + c, rows, :]
        if add is not None:
            r_wait(way, add)
            part = part + rsr[way, add].astype(F32)
        rss[way, k] = part.astype(BF)
        dev = {"x": xp} if way == 0 else {"x": xm}
        send(rss.at[way, k], rsr.at[way, k], n_s.at[way, k], n_r.at[way, k], dev)

    def r_wait(way, k):
        arrived(rsr.at[way, k], n_s.at[way, k], n_r.at[way, k], {"x": xp})

    parts(0, own)
    g(0, 1, 1)
    pair_sum(0, own)
    r_send(0, 0, xa, own)
    r_send(1, 0, xm, own)
    arrived(rdr, rd_s.at[0], rd_r.at[0], to_c)
    rds[1] = rds[0] + rdr[...]
    for k, dev in enumerate(({"x": xp}, {"x": xm}, {"x": xa})):
        send(rds.at[1], rdx.at[k], rd_s.at[1 + k], rd_r.at[1 + k], dev)
    g(1, 0, 2)
    g(1, 0, 1)
    g(0, 2, 2)

    arrived(dl.at[0, oth, :], d_s.at[0], d_r.at[0], to_y)
    parts(1, oth)
    pair_sum(1, oth)
    r_send(1, 1, xa, oth)
    r_send(0, 1, xp, own, 0)
    r_send(0, 2, xp, oth)

    dlt_make(0)
    g(0, 0, 0)
    g(1, 0, 0)
    g(0, 2, 1)
    g(1, 1, 2)
    g(1, 1, 1)
    for k in range(3):
        arrived(rdx.at[k], rd_s.at[1 + k], rd_r.at[1 + k], {"x": xp})
    rds[2] = rds[1] + rdx[0] + rdx[1] + rdx[2]
    send(rds.at[2], rdy, rd_s.at[4], rd_r.at[4], to_y)
    rdb[own, :] = jnp.transpose(jnp.broadcast_to(rds[2, 0:1, :], (HD, B)))
    r_send(1, 2, xm, oth, 1)

    def share(rows, first, second):
        r_wait(*first)
        r_wait(*second)
        nd[rows, :] = npart[t, rows, :] + rsr[first].astype(F32) + rsr[second].astype(F32)
        for hf in range(2):
            cut = pl.ds(hf * HD, HD)
            inv = invb[rows, :]
            v = xr[t, rows, cut].astype(F32)
            n = nd[rows, cut]
            gn = gainf[2 * t + y, :, cut]
            out = xs[1, t, rows, cut].astype(F32) + inv * gn * n - v * (inv * inv) * rdb[rows, :] * (1.0 / D)
            ps[rows, cut] = out.astype(BF)

    def gain_term(rows, cut):
        return jnp.sum(nd[rows, cut] * xr[t, rows, cut].astype(F32) * invb[rows, :], axis=0, keepdims=True)

    across = {"section": psec, "y": py}
    share(own, (0, 1), (1, 0))
    send(ps.at[own, :], rel, ps_s.at[0], ps_r.at[0], across)
    g(0, 3, 2)
    g(0, 1, 0)
    g(1, 1, 0)
    arrived(rdy, rd_s.at[4], rd_r.at[4], to_y)
    rdb[oth, :] = jnp.transpose(jnp.broadcast_to(rdy[0:1, :], (HD, B)))
    share(oth, (0, 2), (1, 2))
    send(ps.at[oth, :], og.at[t, y], ps_s.at[1], ps_r.at[1], across)
    for hf in range(2):
        cut = pl.ds(hf * HD, HD)
        gb[z, :, cut] = jnp.broadcast_to(gain_term(own, cut) + gain_term(oth, cut), (8, HD))

    def gb_send(h):
        blk = lax.rem(z + NZ - h, NZ)
        send(gb.at[blk], gb.at[blk], gb_s.at[0, h], gb_r.at[0, h], {"z": zr_})
        if h < 3:
            blk = lax.rem(z + h, NZ)
            send(gb.at[blk], gb.at[blk], gb_s.at[1, h], gb_r.at[1, h], {"z": zl_})

    def gb_wait(h):
        blk = lax.rem(z + NZ - h, NZ)
        arrived(gb.at[blk], gb_s.at[0, h - 1], gb_r.at[0, h - 1], {"z": zr_})
        if h < 4:
            blk = lax.rem(z + h, NZ)
            arrived(gb.at[blk], gb_s.at[1, h - 1], gb_r.at[1, h - 1], {"z": zl_})

    gb_send(0)
    g(0, 3, 1)
    g(1, 2, 2)

    arrived(rel, ps_s.at[0], ps_r.at[0], across)
    send(rel, og.at[t, py], ps_s.at[2], ps_r.at[2], to_y)
    g(1, 2, 1)
    g(0, 2, 0)

    tr, tl, ta = 2 * xm + c, 2 * xp + c, 2 * xa + c

    def og_send(blk, par, k, dev):
        send(og.at[blk, par], og.at[blk, par], og_s.at[k], og_r.at[k], dev)

    def og_wait(blk, par, k):
        arrived(og.at[blk, par], og_s.at[k], og_r.at[k], to_c)

    arrived(og.at[t, py], ps_s.at[1], ps_r.at[1], across)
    og_send(t, py, 0, {"x": xp})
    og_send(t, py, 1, {"x": xm})
    og_send(t, py, 6, to_c)
    arrived(og.at[t, y], ps_s.at[2], ps_r.at[2], to_y)
    og_send(t, y, 2, {"x": xp})
    og_send(t, y, 3, {"x": xm})
    og_send(t, y, 7, to_c)
    gb_wait(1)
    gb_send(1)
    g(1, 2, 0)
    og_wait(tr, py, 0)
    og_send(tr, py, 4, {"x": xp})
    og_send(tr, py, 8, to_c)
    og_wait(tl, py, 1)
    og_send(tl, py, 9, to_c)
    gb_wait(2)
    gb_send(2)
    og_wait(tl, y, 3)
    og_send(tl, y, 5, {"x": xm})
    og_send(tl, y, 11, to_c)
    og_wait(tr, y, 2)
    og_send(tr, y, 10, to_c)
    g(0, 3, 0)
    gb_wait(3)
    gb_send(3)

    for ch in (2, 1, 0):
        part = weight_part(z, ch)
        for way, last in ((0, 3), (1, 2)):
            g_copy(way, last, ch).wait_recv()
            part = part + gr[way, last, ch].astype(F32)
        part = jnp.transpose(part).astype(BF)
        if ch == 2:
            go[...] = part
        elif ch == 1:
            gq[...] = part
        else:
            gk[...] = part[:, :HD]
            gv[...] = part[:, HD:]

    og_wait(ta, py, 4)
    og_send(ta, py, 12, to_c)
    og_wait(ta, y, 5)
    og_send(ta, y, 13, to_c)

    gb_wait(4)
    gsum = gb[0]
    for i in range(1, NZ):
        gsum = gsum + gb[i]
    gg[y] = gsum
    send(gg.at[y], gg.at[y], gy_s, gy_r, to_y)

    sib = 1 - 2 * c
    for blk, ks in ((t, (6, 7)), (tr, (8, 10)), (tl, (9, 11)), (ta, (12, 13))):
        og_wait(blk + sib, py, ks[0])
        og_wait(blk + sib, y, ks[1])
    arrived(gg.at[py], gy_s, gy_r, to_y)
    for copy in sends:
        copy.wait_send()
    x_out.wait_send()
    u_out.wait_send()


def finish(og, gq, gk, gv, go, gg, passed, oq, ok, ov, oo, gain_sum):
    for blk in range(8):
        for par in range(2):
            at = (2 * blk + par) * B
            passed[0, :, at : at + B] = og[blk, par]
    oq[0] = gq[...]
    ok[0] = gk[...]
    ov[0] = gv[...]
    oo[0] = go[...]
    gain_sum[:, :B] = gg[0, 0:1, :]
    gain_sum[:, B:] = gg[1, 0:1, :]


def tables():
    freq = 10000.0 ** (-2.0 * np.arange(HD // 2) / HD)
    freq = np.concatenate([freq, freq])
    off = np.arange(B)[:, None] * freq[None, :]
    blk = (np.arange(16) * B)[:, None, None] * freq[None, None, :]
    return [a.astype(np.float32) for a in (np.cos(off), np.sin(off), np.cos(blk), np.sin(blk))]


def per_device(layer_input, upstream, norm_gain, query_weight, key_weight, value_weight, output_weight):
    dma = pltpu.SemaphoreType.DMA
    vm = pltpu.VMEM
    scratch = [
        vm((D // B, 1, B), F32), vm((B, B), BF),
        vm((NZ, 3, B, B), BF), vm((2, NZ, 2 * B, B), BF), vm((NZ, 2 * B, B), BF), vm((B, D), BF),
        vm((2 * B, HD), F32), vm((8, B), F32), vm((8, B), F32), vm((3, 2 * B, B), F32),
        vm((3, B, B), BF), vm((3, B, B), BF), vm((B, HD), F32), vm((B, HD), F32),
        vm((2, B, HD), BF), vm((9, 2, B, HD), BF), vm((2, B, HD), BF), vm((2, HD, B), BF), vm((2, HD, B), BF),
        vm((2, 9, B, B), F32), vm((2, 9, B, B), F32),
        vm((2, B, HD), F32), vm((2, B, HD), F32), vm((2, B, HD), F32), vm((2, B, HD), F32), vm((2, B, HD), F32),
        vm((5, 2, HD, B), F32), vm((4, 2, HD, B), BF), vm((4, 2, HD, B), BF), vm((4, 2, HD, B), BF), vm((4, 2, HD, B), BF),
        vm((3, 2 * B, B), BF), vm((3, B, 2 * B), BF),
        vm((3, 8, B), F32), vm((8, B), F32), vm((3, 8, B), F32), vm((8, B), F32), vm((2 * B, HD), F32),
        vm((2, 4, 3, B, B), BF), vm((2, 4, 3, B, B), BF),
        vm((NZ, 2 * B, B), F32), vm((NX, 2 * B, B), BF), vm((NX, 2 * B, B), BF),
        vm((2, 3, B, B), BF), vm((2, 3, B, B), BF), vm((2 * B, B), F32), vm((2 * B, B), BF),
        vm((NZ, 8, B), F32),
        dma((4,)), dma, dma, dma,
        dma((2, 4, 3)), dma((2, 4, 3)), dma((4,)), dma((4,)), dma, dma, dma((3,)), dma((3,)),
        dma((4, 2)), dma((4, 2)), dma((9, 2)), dma((4,)), dma((4,)), dma((4,)), dma((4,)), dma((3,)), dma((3,)),
        dma((5,)), dma((5,)), dma((2, 4, 3)), dma((2, 4, 3)), dma((2, 4)), dma((2, 4)), dma((2, 3)), dma((2, 3)),
        dma((3,)), dma((3,)),
        dma((14,)), dma((14,)), dma((2, 4)), dma((2, 4)), dma, dma,
    ]
    hbm = pl.BlockSpec(memory_space=pl.ANY)
    vmem = pl.BlockSpec(memory_space=pltpu.VMEM)
    og, gq, gk, gv, go, gg = pl.pallas_call(
        kernel,
        out_shape=[
            jax.ShapeDtypeStruct((8, 2, B, B), BF),
            jax.ShapeDtypeStruct((B, B), BF),
            jax.ShapeDtypeStruct((B, HD), BF),
            jax.ShapeDtypeStruct((B, HD), BF),
            jax.ShapeDtypeStruct((B, B), BF),
            jax.ShapeDtypeStruct((2, 8, B), F32),
        ],
        in_specs=[hbm] * 6 + [vmem] * 5,
        out_specs=[vmem] * 6,
        scratch_shapes=scratch,
        compiler_params=pltpu.CompilerParams(
            collective_id=0, has_side_effects=True, vmem_limit_bytes=60 * 1024 * 1024
        ),
        name="step",
    )(
        layer_input[0], upstream[0], query_weight[0], key_weight[0], value_weight[0], output_weight[0],
        norm_gain, *tables(),
    )
    return pl.pallas_call(
        finish,
        out_shape=[
            jax.ShapeDtypeStruct((1, B, D), BF),
            jax.ShapeDtypeStruct((1, B, B), BF),
            jax.ShapeDtypeStruct((1, B, HD), BF),
            jax.ShapeDtypeStruct((1, B, HD), BF),
            jax.ShapeDtypeStruct((1, B, B), BF),
            jax.ShapeDtypeStruct((1, 2 * B), F32),
        ],
        in_specs=[vmem] * 6,
        out_specs=[vmem] * 6,
        name="finish",
    )(og, gq, gk, gv, go, gg)


def solution(mesh):
    split = Mesh(mesh.devices.reshape(2, NZ, 2, NX, 2), AXES)
    seq, tp = ("z", "y"), ("x", "c")
    rows = P("section", seq, None)
    weight = P("section", seq, tp)
    return jax.shard_map(
        per_device,
        mesh=split,
        in_specs=(rows, rows, P("section", None), weight, weight, weight, weight),
        out_specs=(rows, weight, weight, weight, weight, P("section", tp)),
        check_vma=False,
    )
```

```python
import math

import jax
import jax.numpy as jnp
import numpy as np
from jax import lax
from jax.experimental import pallas as pl
from jax.experimental.pallas import tpu as pltpu
from jax.sharding import Mesh
from jax.sharding import PartitionSpec as P

AXES = ("section", "z", "y", "x", "c")
MESH = pl.DeviceIdType.MESH
D = 4096
HD = 128
WINDOW = 2048
B = 256
NZ = 8
NX = 4
EPS = 1e-05
SCALE = 1.0 / math.sqrt(HD)
F32 = jnp.float32
BF = jnp.bfloat16
RIGHT = (4, 3, 4, 3, 4, 3)
LEFT = (3, 4, 3, 4, 3, 4)


def nt(a, b):
    return lax.dot_general(a, b, (((1,), (1,)), ((), ())), preferred_element_type=F32)


def nn(a, b):
    return lax.dot_general(a, b, (((1,), (0,)), ((), ())), preferred_element_type=F32)


def kernel(
    x_hbm, u_hbm, qw, kw, vw, ow, gain, off_c, off_s, blk_c, blk_s,
    og, gq, gk, gv, go, gg,
    gainf, rel, wbuf, xs, xr, xin, invb, isend, irecv, acc, pbuf, rbuf, cosb, sinb,
    qb, kv, dob, qt, dot_, sb, db, msl, mb, lb, oacc, dqa, delta,
    dkve, ysrc, yrcv, zsrc, zrcv, dl, dlt, rds, rdr, rdx, rdy, rdb,
    gs, gr, npart, cs, cr, rss, rsr, nd, ps, gb,
    l_w, l_x, l_u, l_r,
    w_s, w_r, x_s, x_r, i_s, i_r, p_s, p_r,
    kz_s, ky_s, kv_r, yr_s, yr_r, zr_s, zr_r, d_s, d_r,
    rd_s, rd_r, g_s, g_r, c_s, c_r, n_s, n_r, ps_s, ps_r,
    og_s, og_r, gb_s, gb_r, gy_s, gy_r,
):
    sec = lax.axis_index("section")
    z = lax.axis_index("z")
    y = lax.axis_index("y")
    x = lax.axis_index("x")
    c = lax.axis_index("c")
    s = 2 * z + y
    t = 2 * x + c
    zr_, zl_ = lax.rem(z + 1, NZ), lax.rem(z + NZ - 1, NZ)
    xp, xm, xa = lax.rem(x + 1, NX), lax.rem(x + NX - 1, NX), lax.rem(x + 2, NX)
    py, pc, psec = 1 - y, 1 - c, 1 - sec
    to_y = {"y": py}
    to_c = {"c": pc}
    own = pl.ds(pl.multiple_of(y * B, B), B)
    oth = pl.ds(pl.multiple_of(py * B, B), B)

    def rc(src, dst, ss, rs, dev):
        return pltpu.make_async_remote_copy(
            src_ref=src, dst_ref=dst, send_sem=ss, recv_sem=rs,
            device_id=dev, device_id_type=MESH,
        )

    sends = []

    def send(src, dst, ss, rs, dev):
        copy = rc(src, dst, ss, rs, dev)
        copy.start()
        sends.append(copy)
        return copy

    def arrived(dst, ss, rs, dev):
        rc(dst, dst, ss, rs, dev).wait_recv()

    loads = [
        pltpu.make_async_copy(kw, wbuf.at[z, 0, :, pl.ds(0, HD)], l_w.at[0]),
        pltpu.make_async_copy(vw, wbuf.at[z, 0, :, pl.ds(HD, HD)], l_w.at[1]),
        pltpu.make_async_copy(qw, wbuf.at[z, 1], l_w.at[2]),
        pltpu.make_async_copy(ow, wbuf.at[z, 2], l_w.at[3]),
        pltpu.make_async_copy(x_hbm, xin, l_x),
    ]
    for copy in loads:
        copy.start()

    def cols(blk, parity):
        return pl.ds(pl.multiple_of((2 * blk + parity) * B, B), B)

    for j in range(NZ):
        pltpu.make_async_copy(u_hbm.at[:, cols(j, y)], xs.at[1, j, own, :], l_u).start()
        pltpu.make_async_copy(x_hbm.at[:, cols(j, y)], xr.at[j, own, :], l_r).start()

    barrier = pltpu.get_barrier_semaphore()
    greet = [
        {"z": zr_}, {"z": zl_}, to_y, to_c, {"x": xp}, {"x": xm}, {"x": xa},
        {"section": psec, "y": py},
    ]
    for dev in greet:
        pl.semaphore_signal(barrier, inc=1, device_id=dev, device_id_type=MESH)
    pl.semaphore_wait(barrier, len(greet))

    for copy in loads[:4]:
        copy.wait()

    def w_half(blk, n):
        return wbuf.at[blk, n // 2, :, pl.ds(n % 2 * HD, HD)]

    def w_copy(way, h, n):
        blk = lax.rem(z + NZ - h, NZ) if way == 0 else lax.rem(z + h, NZ)
        dev = {"z": zr_ if way == 0 else zl_}
        return rc(w_half(blk, n), w_half(blk, n), w_s.at[way, h, n], w_r.at[way, h, n], dev)

    def w_send(h, n):
        for way, hops in ((0, RIGHT), (1, LEFT)):
            if h < hops[n]:
                copy = w_copy(way, h, n)
                copy.start()
                sends.append(copy)

    def w_wait(h, n):
        for way, hops in ((0, RIGHT), (1, LEFT)):
            if h <= hops[n]:
                blk = lax.rem(z + NZ - h, NZ) if way == 0 else lax.rem(z + h, NZ)
                arrived(w_half(blk, n), w_s.at[way, h - 1, n], w_r.at[way, h - 1, n], {"z": zr_})

    def w_hop(h, halves):
        for n in halves:
            w_wait(h, n)
            w_send(h, n)

    early, late = (0, 1, 2), (3, 4, 5)
    for n in early:
        w_send(0, n)

    mine = pl.ds(pl.multiple_of(c * 128, 128), 128)
    there = pl.ds(pl.multiple_of(y * B + c * 128, 128), 128)
    from_y = pl.ds(pl.multiple_of(py * B + c * 128, 128), 128)
    from_c = pl.ds(pl.multiple_of(py * B + pc * 128, 128), 128)
    for j in range(NZ):
        rc(x_hbm.at[mine, cols(j, py)], xr.at[j, there, :], x_s.at[0], x_r.at[0], to_y).start()

    def u_start(part):
        for j in range(4 * part, 4 * part + 4):
            dst = xs.at[1, j, there, :]
            rc(u_hbm.at[mine, cols(j, py)], dst, x_s.at[1 + part], x_r.at[1 + part], to_y).start()

    def u_rows(part, rows):
        return xs.at[1, pl.ds(4 * part, 4), rows, :]

    u_start(0)
    x_out = rc(xr.at[:, from_y, :], xr.at[:, there, :], x_s.at[0], x_r.at[0], to_y)
    u_out = [
        rc(u_rows(p, from_y), u_rows(p, there), x_s.at[1 + p], x_r.at[1 + p], to_y) for p in range(2)
    ]

    def u_take(part):
        u_out[part].wait_recv()
        send(u_rows(part, from_y), u_rows(part, from_y), x_s.at[4 + part], x_r.at[4 + part], to_c)

    for j in range(D // B):
        gainf[j] = gain[:, j * B : (j + 1) * B].astype(F32)

    lane = lax.broadcasted_iota(jnp.int32, (B, HD), 1)
    cosb[...] = blk_c[s] * off_c[...] - blk_s[s] * off_s[...]
    sin_all = blk_s[s] * off_c[...] + blk_c[s] * off_s[...]
    sinb[...] = jnp.where(lane < HD // 2, -sin_all, sin_all)

    loads[4].wait()
    invb[own, :] = jnp.zeros((B, HD), F32)

    def squares(j, _):
        v = xin[:, pl.ds(pl.multiple_of(j * B, B), B)].astype(F32)
        invb[own, :] += v[:, :HD] * v[:, :HD] + v[:, HD:] * v[:, HD:]
        return 0

    lax.fori_loop(0, D // B, squares, 0)
    mean = jnp.sum(invb[own, :], axis=1, keepdims=True) / D
    inv_own = jnp.broadcast_to(lax.rsqrt(mean + EPS), (B, HD))
    invb[own, :] = inv_own
    isend[...] = jnp.transpose(inv_own)[:8, :]
    send(isend, irecv, i_s, i_r, to_y)

    whole = pltpu.make_async_copy(xs.at[1, :, oth, :], xs.at[1, :, own, :], l_u)
    whole.wait()
    pltpu.make_async_copy(xr.at[:, oth, :], xr.at[:, own, :], l_r).wait()

    def norm_rows(rows):
        def step(j, _):
            inv = invb[rows, :]
            g = gainf[2 * j + y]
            v = xr[j, rows, :].astype(F32)
            n = jnp.concatenate([v[:, :HD] * inv, v[:, HD:] * inv], axis=1) * g
            xs[0, j, rows, :] = n.astype(BF)
            return 0

        lax.fori_loop(0, NZ, step, 0)

    norm_rows(own)

    for h in (1, 2, 3):
        w_hop(h, early)
    for n in late:
        w_send(0, n)
    x_out.wait_recv()
    send(xr.at[:, from_y, :], xr.at[:, from_y, :], x_s.at[3], x_r.at[3], to_c)

    arrived(irecv, i_s, i_r, to_y)
    inv_oth = jnp.transpose(jnp.broadcast_to(irecv[0:1, :], (HD, B)))
    invb[oth, :] = inv_oth
    arrived(xr.at[:, from_c, :], x_s.at[3], x_r.at[3], to_c)
    norm_rows(oth)

    def project(ch, lo, hi):
        def step(n, _):
            blk = lax.rem(z + 5 + n, NZ)
            acc[ch] += nn(xs[1 if ch == 2 else 0, blk], wbuf[blk, ch])
            return 0

        if lo == 0:
            acc[ch] = jnp.zeros((2 * B, B), F32)
        lax.fori_loop(lo, hi, step, 0)

    def p_copy(ch):
        return rc(pbuf.at[ch], rbuf.at[ch], p_s.at[ch], p_r.at[ch], to_y)

    def project_out(ch):
        pbuf[ch] = acc[ch, oth, :].astype(BF)
        p_copy(ch).start()
        sends.append(p_copy(ch))

    def total(ch):
        p_copy(ch).wait_recv()
        return acc[ch, own, :] + rbuf[ch].astype(F32)

    def rot(v, sign):
        return v * cosb[...] + pltpu.roll(v, HD // 2, 1) * (sign * sinb[...])

    project(0, 0, 7)
    for n in early:
        w_wait(4, n)
    project(0, 7, 8)
    project_out(0)
    u_start(1)
    w_hop(1, late)
    u_take(0)
    both = total(0)
    kv[0, 0] = rot(both[:, :HD], 1.0).astype(BF)
    kv[0, 1] = both[:, HD:].astype(BF)

    def kz_send(i, k):
        send(kv.at[2 * i, k], kv.at[2 * i + 2, k], kz_s.at[i, k], kv_r.at[2 * i + 2, k], {"z": zr_})

    def ky_copy(i, k):
        return rc(kv.at[2 * i + 2 * y, k], kv.at[2 * i + 1, k], ky_s.at[i, k], kv_r.at[2 * i + 1, k], to_y)

    def ky_start(i, k, side):
        @pl.when(y == side)
        def _():
            ky_copy(i, k).start()

    for k in range(2):
        kz_send(0, k)
        ky_start(0, k, 0)

    def halo(i):
        for k in range(2):
            arrived(kv.at[2 * i + 2, k], kz_s.at[i, k], kv_r.at[2 * i + 2, k], {"z": zr_})
            if i < 3:
                kz_send(i + 1, k)
                ky_start(i + 1, k, 0)
            ky_start(i, k, 1)

    def halo_odd(i):
        for k in range(2):
            arrived(kv.at[2 * i + 1, k], ky_s.at[i, k], kv_r.at[2 * i + 1, k], to_y)
            sends.append(ky_copy(i, k))

    w_hop(2, late)
    halo(0)
    u_take(1)
    w_hop(3, late)
    halo(1)
    project(1, 0, 7)
    for n in late:
        w_wait(4, n)
    project(1, 7, 8)
    project_out(1)
    halo(2)
    for p in range(2):
        arrived(u_rows(p, from_c), x_s.at[4 + p], x_r.at[4 + p], to_c)
    project(2, 0, 8)
    project_out(2)
    halo(3)

    for h in range(2):
        mb[h] = jnp.full((B, HD), -3e38, F32)
        lb[h] = jnp.zeros((B, HD), F32)
        oacc[h] = jnp.zeros((B, HD), F32)
        dqa[h] = jnp.zeros((B, HD), F32)
    both = total(1)
    for h in range(2):
        q = rot(both[:, h * HD : (h + 1) * HD], 1.0)
        qb[h] = q.astype(BF)
        qt[h] = jnp.transpose(q).astype(BF)
    both = total(2)
    for h in range(2):
        v = both[:, h * HD : (h + 1) * HD]
        dob[h] = v.astype(BF)
        dot_[h] = jnp.transpose(v).astype(BF)

    diff = lax.broadcasted_iota(jnp.int32, (B, B), 1) - lax.broadcasted_iota(jnp.int32, (B, B), 0)

    def attend(d, _):
        top = jnp.where(s >= d, d * B, -2 * WINDOW)
        allowed = (diff <= top) & (diff > d * B - WINDOW)
        for h in range(2):
            sc = jnp.where(allowed, nt(qb[h], kv[d, 0]) * SCALE, -1e30)
            db[h, d] = nt(dob[h], kv[d, 1])
            before = mb[h]
            peak = jnp.max(jnp.maximum(sc[:, :HD], sc[:, HD:]), axis=1, keepdims=True)
            now = jnp.maximum(before, peak)
            e = jnp.exp(sc - jnp.concatenate([now, now], axis=1))
            keep = jnp.exp(before - now)
            sb[h, d] = e
            mb[h] = now
            msl[h, d] = now
            lb[h] = lb[h] * keep + e[:, :HD] + e[:, HD:]
            oacc[h] = oacc[h] * keep + nn(e.astype(BF), kv[d, 1])
        return 0

    lax.fori_loop(0, 1, attend, 0)
    for i in range(3):
        halo_odd(i)
    lax.fori_loop(1, 7, attend, 0)
    halo_odd(3)
    lax.fori_loop(7, 9, attend, 0)

    for h in range(2):
        scale = jnp.broadcast_to(1.0 / jnp.sum(lb[h], axis=1, keepdims=True), (B, HD))
        lb[h] = scale
        att = (oacc[h] * scale).astype(BF)
        dl[2, own, pl.ds(h * HD, HD)] = att
        delta[h] = jnp.broadcast_to(
            jnp.sum(att.astype(F32) * dob[h].astype(F32), axis=1, keepdims=True), (B, HD)
        )

    def dl_send(ch):
        send(dl.at[ch, own, :], dl.at[ch, own, :], d_s.at[ch], d_r.at[ch], to_y)

    dl_send(2)

    def slot_grads(d):
        dkt = jnp.zeros((HD, B), F32)
        dvt = jnp.zeros((HD, B), F32)
        for h in range(2):
            f = jnp.exp(msl[h, d] - mb[h]) * lb[h]
            p = sb[h, d] * jnp.concatenate([f, f], axis=1)
            r = delta[h]
            ds = (p * (db[h, d] - jnp.concatenate([r, r], axis=1)) * SCALE).astype(BF)
            dqa[h] += nn(ds, kv[d, 0])
            dkt = dkt + nn(qt[h], ds)
            dvt = dvt + nn(dot_[h], p.astype(BF))
        return dkt, dvt

    def y_copy(i, k):
        return rc(ysrc.at[i, k], yrcv.at[i, k], yr_s.at[i, k], yr_r.at[i, k], to_y)

    def slot_pair(i):
        for k, part in enumerate(slot_grads(2 * i + 1)):
            ysrc[i, k] = part.astype(BF)
            y_copy(i, k).start()
            sends.append(y_copy(i, k))
        for k, part in enumerate(slot_grads(2 * i + 2)):
            dkve[i + 1, k] = part

    def from_partner(e, k):
        i = e // 2 - y
        keep = jnp.where((i >= 0) & (i < 4), 1.0, 0.0)
        return yrcv[jnp.clip(i, 0, 3), k].astype(F32) * keep

    def chain_sum(i, k):
        e = 8 - 2 * i
        if i < 4:
            y_copy(3 - i, k).wait_recv()
        part = dkve[e // 2, k] + from_partner(e, k)
        if i > 0:
            arrived(zrcv.at[i - 1, k], zr_s.at[i - 1, k], zr_r.at[i - 1, k], {"z": zl_})
            part = part + zrcv[i - 1, k].astype(F32)
        return part

    def chain(i):
        for k in range(2):
            zsrc[i, k] = chain_sum(i, k).astype(BF)
            send(zsrc.at[i, k], zrcv.at[i, k], zr_s.at[i, k], zr_r.at[i, k], {"z": zl_})

    def dlt_make(ch):
        dlt[ch] = jnp.transpose(dl[ch].astype(F32)).astype(BF)

    def g_copy(way, j, ch):
        dev = {"z": zr_ if way == 0 else zl_}
        return rc(gs.at[way, j, ch], gr.at[way, j, ch], g_s.at[way, j, ch], g_r.at[way, j, ch], dev)

    def weight_part(blk, ch):
        return nn(dlt[ch], xs[1 if ch == 2 else 0, blk])

    def g(way, j, ch):
        step = 4 - j if way == 0 else NZ - (3 - j)
        part = weight_part(lax.rem(z + step, NZ), ch)
        if j > 0:
            g_copy(way, j - 1, ch).wait_recv()
            part = part + gr[way, j - 1, ch].astype(F32)
        gs[way, j, ch] = part.astype(BF)
        copy = g_copy(way, j, ch)
        copy.start()
        sends.append(copy)

    def query_parts(b, _):
        npart[b] = nt(dl[1], wbuf[b, 1])
        return 0

    for i in (3, 2, 1, 0):
        slot_pair(i)
    for k, part in enumerate(slot_grads(0)):
        dkve[0, k] = part
    for h in range(2):
        dl[1, own, pl.ds(h * HD, HD)] = rot(dqa[h], -1.0).astype(BF)
    chain(0)
    dl_send(1)
    arrived(dl.at[2, oth, :], d_s.at[2], d_r.at[2], to_y)
    dlt_make(2)
    g(0, 0, 2)
    chain(1)
    arrived(dl.at[1, oth, :], d_s.at[1], d_r.at[1], to_y)
    dlt_make(1)
    g(0, 0, 1)
    chain(2)
    lax.fori_loop(0, NZ, query_parts, 0)
    chain(3)
    g(0, 1, 2)
    g(0, 1, 1)

    dk = jnp.transpose(chain_sum(4, 0))
    dv = jnp.transpose(chain_sum(4, 1))
    dl[0, own, pl.ds(0, HD)] = rot(dk, -1.0).astype(BF)
    dl[0, own, pl.ds(HD, HD)] = dv.astype(BF)
    dl_send(0)

    rd = dk * kv[0, 0].astype(F32) + dv * kv[0, 1].astype(F32)
    for h in range(2):
        rd = rd + dqa[h] * qb[h].astype(F32)
    rd = jnp.broadcast_to(jnp.sum(rd, axis=1, keepdims=True), (B, HD))
    rds[0] = jnp.transpose(rd)[:8, :]
    send(rds.at[0], rdr, rd_s.at[0], rd_r.at[0], to_c)

    def c_copy(k, i, rows):
        return rc(cs.at[i, rows, :], cr.at[i, rows, :], c_s.at[k, i], c_r.at[k, i], to_c)

    def parts(k, rows):
        def out(i, _):
            b = 2 * i + pc
            cs[i, rows, :] = (npart[b, rows, :] + nt(dl[0, rows, :], wbuf[b, 0])).astype(BF)
            c_copy(k, i, rows).start()
            return 0

        def keep(i, _):
            b = 2 * i + c
            npart[b, rows, :] += nt(dl[0, rows, :], wbuf[b, 0])
            return 0

        lax.fori_loop(0, NX, out, 0)
        lax.fori_loop(0, NX, keep, 0)
        for i in range(NX):
            sends.append(c_copy(k, i, rows))

    def pair_sum(k, rows):
        for i in range(NX):
            c_copy(k, i, rows).wait_recv()

        def add(i, _):
            npart[2 * i + c, rows, :] += cr[i, rows, :].astype(F32)
            return 0

        lax.fori_loop(0, NX, add, 0)

    def r_send(way, k, blk, rows, add=None):
        part = npart[2 * blk + c, rows, :]
        if add is not None:
            r_wait(way, add)
            part = part + rsr[way, add].astype(F32)
        rss[way, k] = part.astype(BF)
        dev = {"x": xp} if way == 0 else {"x": xm}
        send(rss.at[way, k], rsr.at[way, k], n_s.at[way, k], n_r.at[way, k], dev)

    def r_wait(way, k):
        arrived(rsr.at[way, k], n_s.at[way, k], n_r.at[way, k], {"x": xp})

    parts(0, own)
    pair_sum(0, own)
    r_send(0, 0, xa, own)
    r_send(1, 0, xm, own)
    arrived(rdr, rd_s.at[0], rd_r.at[0], to_c)
    rds[1] = rds[0] + rdr[...]
    for k, dev in enumerate(({"x": xp}, {"x": xm}, {"x": xa})):
        send(rds.at[1], rdx.at[k], rd_s.at[1 + k], rd_r.at[1 + k], dev)
    g(1, 0, 2)
    g(1, 0, 1)
    g(0, 2, 2)

    arrived(dl.at[0, oth, :], d_s.at[0], d_r.at[0], to_y)
    parts(1, oth)
    pair_sum(1, oth)
    r_send(1, 1, xa, oth)
    r_send(0, 1, xp, own, 0)
    r_send(0, 2, xp, oth)

    dlt_make(0)
    g(0, 0, 0)
    g(1, 0, 0)
    g(0, 2, 1)
    g(1, 1, 2)
    g(1, 1, 1)
    for k in range(3):
        arrived(rdx.at[k], rd_s.at[1 + k], rd_r.at[1 + k], {"x": xp})
    rds[2] = rds[1] + rdx[0] + rdx[1] + rdx[2]
    send(rds.at[2], rdy, rd_s.at[4], rd_r.at[4], to_y)
    rdb[own, :] = jnp.transpose(jnp.broadcast_to(rds[2, 0:1, :], (HD, B)))
    r_send(1, 2, xm, oth, 1)

    def share(rows, first, second):
        r_wait(*first)
        r_wait(*second)
        nd[rows, :] = npart[t, rows, :] + rsr[first].astype(F32) + rsr[second].astype(F32)
        for hf in range(2):
            cut = pl.ds(hf * HD, HD)
            inv = invb[rows, :]
            v = xr[t, rows, cut].astype(F32)
            n = nd[rows, cut]
            gn = gainf[2 * t + y, :, cut]
            out = xs[1, t, rows, cut].astype(F32) + inv * gn * n - v * (inv * inv) * rdb[rows, :] * (1.0 / D)
            ps[rows, cut] = out.astype(BF)

    def gain_term(rows, cut):
        return jnp.sum(nd[rows, cut] * xr[t, rows, cut].astype(F32) * invb[rows, :], axis=0, keepdims=True)

    across = {"section": psec, "y": py}
    share(own, (0, 1), (1, 0))
    send(ps.at[own, :], rel, ps_s.at[0], ps_r.at[0], across)
    g(0, 3, 2)
    g(0, 1, 0)
    g(1, 1, 0)
    arrived(rdy, rd_s.at[4], rd_r.at[4], to_y)
    rdb[oth, :] = jnp.transpose(jnp.broadcast_to(rdy[0:1, :], (HD, B)))
    share(oth, (0, 2), (1, 2))
    send(ps.at[oth, :], og.at[t, y], ps_s.at[1], ps_r.at[1], across)
    for hf in range(2):
        cut = pl.ds(hf * HD, HD)
        gb[z, :, cut] = jnp.broadcast_to(gain_term(own, cut) + gain_term(oth, cut), (8, HD))

    def gb_send(h):
        blk = lax.rem(z + NZ - h, NZ)
        send(gb.at[blk], gb.at[blk], gb_s.at[0, h], gb_r.at[0, h], {"z": zr_})
        if h < 3:
            blk = lax.rem(z + h, NZ)
            send(gb.at[blk], gb.at[blk], gb_s.at[1, h], gb_r.at[1, h], {"z": zl_})

    def gb_wait(h):
        blk = lax.rem(z + NZ - h, NZ)
        arrived(gb.at[blk], gb_s.at[0, h - 1], gb_r.at[0, h - 1], {"z": zr_})
        if h < 4:
            blk = lax.rem(z + h, NZ)
            arrived(gb.at[blk], gb_s.at[1, h - 1], gb_r.at[1, h - 1], {"z": zl_})

    gb_send(0)
    g(0, 3, 1)
    g(1, 2, 2)

    arrived(rel, ps_s.at[0], ps_r.at[0], across)
    send(rel, og.at[t, py], ps_s.at[2], ps_r.at[2], to_y)
    g(1, 2, 1)
    g(0, 2, 0)

    tr, tl, ta = 2 * xm + c, 2 * xp + c, 2 * xa + c

    def og_send(blk, par, k, dev):
        send(og.at[blk, par], og.at[blk, par], og_s.at[k], og_r.at[k], dev)

    def og_wait(blk, par, k):
        arrived(og.at[blk, par], og_s.at[k], og_r.at[k], to_c)

    arrived(og.at[t, py], ps_s.at[1], ps_r.at[1], across)
    og_send(t, py, 0, {"x": xp})
    og_send(t, py, 1, {"x": xm})
    og_send(t, py, 6, to_c)
    arrived(og.at[t, y], ps_s.at[2], ps_r.at[2], to_y)
    og_send(t, y, 2, {"x": xp})
    og_send(t, y, 3, {"x": xm})
    og_send(t, y, 7, to_c)
    gb_wait(1)
    gb_send(1)
    g(1, 2, 0)
    og_wait(tr, py, 0)
    og_send(tr, py, 4, {"x": xp})
    og_send(tr, py, 8, to_c)
    og_wait(tl, py, 1)
    og_send(tl, py, 9, to_c)
    gb_wait(2)
    gb_send(2)
    og_wait(tl, y, 3)
    og_send(tl, y, 5, {"x": xm})
    og_send(tl, y, 11, to_c)
    og_wait(tr, y, 2)
    og_send(tr, y, 10, to_c)
    g(0, 3, 0)
    gb_wait(3)
    gb_send(3)

    for ch in (2, 1, 0):
        part = weight_part(z, ch)
        for way, last in ((0, 3), (1, 2)):
            g_copy(way, last, ch).wait_recv()
            part = part + gr[way, last, ch].astype(F32)
        part = jnp.transpose(part).astype(BF)
        if ch == 2:
            go[...] = part
        elif ch == 1:
            gq[...] = part
        else:
            gk[...] = part[:, :HD]
            gv[...] = part[:, HD:]

    og_wait(ta, py, 4)
    og_send(ta, py, 12, to_c)
    og_wait(ta, y, 5)
    og_send(ta, y, 13, to_c)

    gb_wait(4)
    gsum = gb[0]
    for i in range(1, NZ):
        gsum = gsum + gb[i]
    gg[y] = gsum
    send(gg.at[y], gg.at[y], gy_s, gy_r, to_y)

    sib = 1 - 2 * c
    for blk, ks in ((t, (6, 7)), (tr, (8, 10)), (tl, (9, 11)), (ta, (12, 13))):
        og_wait(blk + sib, py, ks[0])
        og_wait(blk + sib, y, ks[1])
    arrived(gg.at[py], gy_s, gy_r, to_y)
    for copy in sends:
        copy.wait_send()
    x_out.wait_send()
    for copy in u_out:
        copy.wait_send()


def finish(og, gq, gk, gv, go, gg, passed, oq, ok, ov, oo, gain_sum):
    for blk in range(8):
        for par in range(2):
            at = (2 * blk + par) * B
            passed[0, :, at : at + B] = og[blk, par]
    oq[0] = gq[...]
    ok[0] = gk[...]
    ov[0] = gv[...]
    oo[0] = go[...]
    gain_sum[:, :B] = gg[0, 0:1, :]
    gain_sum[:, B:] = gg[1, 0:1, :]


def tables():
    freq = 10000.0 ** (-2.0 * np.arange(HD // 2) / HD)
    freq = np.concatenate([freq, freq])
    off = np.arange(B)[:, None] * freq[None, :]
    blk = (np.arange(16) * B)[:, None, None] * freq[None, None, :]
    return [a.astype(np.float32) for a in (np.cos(off), np.sin(off), np.cos(blk), np.sin(blk))]


def per_device(layer_input, upstream, norm_gain, query_weight, key_weight, value_weight, output_weight):
    dma = pltpu.SemaphoreType.DMA
    vm = pltpu.VMEM
    scratch = [
        vm((D // B, 1, B), F32), vm((B, B), BF),
        vm((NZ, 3, B, B), BF), vm((2, NZ, 2 * B, B), BF), vm((NZ, 2 * B, B), BF), vm((B, D), BF),
        vm((2 * B, HD), F32), vm((8, B), F32), vm((8, B), F32), vm((3, 2 * B, B), F32),
        vm((3, B, B), BF), vm((3, B, B), BF), vm((B, HD), F32), vm((B, HD), F32),
        vm((2, B, HD), BF), vm((9, 2, B, HD), BF), vm((2, B, HD), BF), vm((2, HD, B), BF), vm((2, HD, B), BF),
        vm((2, 9, B, B), F32), vm((2, 9, B, B), F32), vm((2, 9, B, HD), F32),
        vm((2, B, HD), F32), vm((2, B, HD), F32), vm((2, B, HD), F32), vm((2, B, HD), F32), vm((2, B, HD), F32),
        vm((5, 2, HD, B), F32), vm((4, 2, HD, B), BF), vm((4, 2, HD, B), BF), vm((4, 2, HD, B), BF), vm((4, 2, HD, B), BF),
        vm((3, 2 * B, B), BF), vm((3, B, 2 * B), BF),
        vm((3, 8, B), F32), vm((8, B), F32), vm((3, 8, B), F32), vm((8, B), F32), vm((2 * B, HD), F32),
        vm((2, 4, 3, B, B), BF), vm((2, 4, 3, B, B), BF),
        vm((NZ, 2 * B, B), F32), vm((NX, 2 * B, B), BF), vm((NX, 2 * B, B), BF),
        vm((2, 3, B, B), BF), vm((2, 3, B, B), BF), vm((2 * B, B), F32), vm((2 * B, B), BF),
        vm((NZ, 8, B), F32),
        dma((4,)), dma, dma, dma,
        dma((2, 4, 6)), dma((2, 4, 6)), dma((6,)), dma((6,)), dma, dma, dma((3,)), dma((3,)),
        dma((4, 2)), dma((4, 2)), dma((9, 2)), dma((4, 2)), dma((4, 2)), dma((4, 2)), dma((4, 2)), dma((3,)), dma((3,)),
        dma((5,)), dma((5,)), dma((2, 4, 3)), dma((2, 4, 3)), dma((2, 4)), dma((2, 4)), dma((2, 3)), dma((2, 3)),
        dma((3,)), dma((3,)),
        dma((14,)), dma((14,)), dma((2, 4)), dma((2, 4)), dma, dma,
    ]
    hbm = pl.BlockSpec(memory_space=pl.ANY)
    vmem = pl.BlockSpec(memory_space=pltpu.VMEM)
    og, gq, gk, gv, go, gg = pl.pallas_call(
        kernel,
        out_shape=[
            jax.ShapeDtypeStruct((8, 2, B, B), BF),
            jax.ShapeDtypeStruct((B, B), BF),
            jax.ShapeDtypeStruct((B, HD), BF),
            jax.ShapeDtypeStruct((B, HD), BF),
            jax.ShapeDtypeStruct((B, B), BF),
            jax.ShapeDtypeStruct((2, 8, B), F32),
        ],
        in_specs=[hbm] * 6 + [vmem] * 5,
        out_specs=[vmem] * 6,
        scratch_shapes=scratch,
        compiler_params=pltpu.CompilerParams(
            collective_id=0, has_side_effects=True, vmem_limit_bytes=60 * 1024 * 1024
        ),
        name="step",
    )(
        layer_input[0], upstream[0], query_weight[0], key_weight[0], value_weight[0], output_weight[0],
        norm_gain, *tables(),
    )
    return pl.pallas_call(
        finish,
        out_shape=[
            jax.ShapeDtypeStruct((1, B, D), BF),
            jax.ShapeDtypeStruct((1, B, B), BF),
            jax.ShapeDtypeStruct((1, B, HD), BF),
            jax.ShapeDtypeStruct((1, B, HD), BF),
            jax.ShapeDtypeStruct((1, B, B), BF),
            jax.ShapeDtypeStruct((1, 2 * B), F32),
        ],
        in_specs=[vmem] * 6,
        out_specs=[vmem] * 6,
        name="finish",
    )(og, gq, gk, gv, go, gg)


def solution(mesh):
    split = Mesh(mesh.devices.reshape(2, NZ, 2, NX, 2), AXES)
    seq, tp = ("z", "y"), ("x", "c")
    rows = P("section", seq, None)
    weight = P("section", seq, tp)
    return jax.shard_map(
        per_device,
        mesh=split,
        in_specs=(rows, rows, P("section", None), weight, weight, weight, weight),
        out_specs=(rows, weight, weight, weight, weight, P("section", tp)),
        check_vma=False,
    )
```

```python
import math

import jax
import jax.numpy as jnp
import numpy as np
from jax import lax
from jax.experimental import pallas as pl
from jax.experimental.pallas import tpu as pltpu
from jax.sharding import Mesh
from jax.sharding import PartitionSpec as P

AXES = ("section", "z", "y", "x", "c")
MESH = pl.DeviceIdType.MESH
D = 4096
HD = 128
WINDOW = 2048
B = 256
NZ = 8
NX = 4
EPS = 1e-05
SCALE = 1.0 / math.sqrt(HD)
F32 = jnp.float32
BF = jnp.bfloat16
RIGHT = (4, 3, 4, 3, 3, 3)
LEFT = (3, 4, 3, 4, 4, 4)


def nt(a, b):
    return lax.dot_general(a, b, (((1,), (1,)), ((), ())), preferred_element_type=F32)


def nn(a, b):
    return lax.dot_general(a, b, (((1,), (0,)), ((), ())), preferred_element_type=F32)


def kernel(
    x_hbm, u_hbm, qw, kw, vw, ow, gain_hbm, off_hbm, blk_hbm,
    og, gq, gk, gv, go, gg,
    gain, off, turn, gainf, rel, wbuf, xs, xr, xin, invb, isend, irecv, acc, pbuf, rbuf, cosb, sinb,
    qb, kv, dob, qt, dot_, sb, msl, mb, lb, oacc, dqa, delta,
    dkve, ysrc, yrcv, zsrc, zrcv, dl, dlt, rds, rdr, rdx, rdy, rdb,
    gs, gr, npart, cs, cr, rss, rsr, nd, ps, gb,
    l_w, l_x, l_u, l_r,
    w_s, w_r, x_s, x_r, i_s, i_r, p_s, p_r,
    kz_s, ky_s, kv_r, yr_s, yr_r, zr_s, zr_r, d_s, d_r,
    rd_s, rd_r, g_s, g_r, c_s, c_r, n_s, n_r, ps_s, ps_r,
    og_s, og_r, gb_s, gb_r, gy_s, gy_r,
):
    sec = lax.axis_index("section")
    z = lax.axis_index("z")
    y = lax.axis_index("y")
    x = lax.axis_index("x")
    c = lax.axis_index("c")
    s = 2 * z + y
    t = 2 * x + c
    zr_, zl_ = lax.rem(z + 1, NZ), lax.rem(z + NZ - 1, NZ)
    xp, xm, xa = lax.rem(x + 1, NX), lax.rem(x + NX - 1, NX), lax.rem(x + 2, NX)
    py, pc, psec = 1 - y, 1 - c, 1 - sec
    to_y = {"y": py}
    to_c = {"c": pc}
    own = pl.ds(pl.multiple_of(y * B, B), B)
    oth = pl.ds(pl.multiple_of(py * B, B), B)

    def rc(src, dst, ss, rs, dev):
        return pltpu.make_async_remote_copy(
            src_ref=src, dst_ref=dst, send_sem=ss, recv_sem=rs,
            device_id=dev, device_id_type=MESH,
        )

    sends = []
    marks = [0, 0]

    def drain():
        for copy in sends[marks[0] : marks[1]]:
            copy.wait_send()
        marks[:] = [marks[1], len(sends)]

    def send(src, dst, ss, rs, dev):
        copy = rc(src, dst, ss, rs, dev)
        copy.start()
        sends.append(copy)
        return copy

    def arrived(dst, ss, rs, dev):
        rc(dst, dst, ss, rs, dev).wait_recv()

    loads = [
        pltpu.make_async_copy(kw, wbuf.at[z, 0, :, pl.ds(0, HD)], l_w.at[0]),
        pltpu.make_async_copy(vw, wbuf.at[z, 0, :, pl.ds(HD, HD)], l_w.at[1]),
        pltpu.make_async_copy(qw, wbuf.at[z, 1], l_w.at[2]),
        pltpu.make_async_copy(ow, wbuf.at[z, 2], l_w.at[3]),
        pltpu.make_async_copy(x_hbm, xin, l_x),
        pltpu.make_async_copy(gain_hbm, gain, l_w.at[4]),
        pltpu.make_async_copy(off_hbm, off, l_w.at[5]),
        pltpu.make_async_copy(blk_hbm, turn, l_w.at[6]),
    ]
    for copy in loads:
        copy.start()

    def cols(blk, parity):
        return pl.ds(pl.multiple_of((2 * blk + parity) * B, B), B)

    for j in range(NZ):
        pltpu.make_async_copy(u_hbm.at[:, cols(j, y)], xs.at[1, j, own, :], l_u).start()
        pltpu.make_async_copy(x_hbm.at[:, cols(j, y)], xr.at[j, own, :], l_r).start()

    barrier = pltpu.get_barrier_semaphore()
    greet = [
        {"z": zr_}, {"z": zl_}, to_y, to_c, {"x": xp}, {"x": xm}, {"x": xa},
        {"section": psec, "y": py},
    ]
    for dev in greet:
        pl.semaphore_signal(barrier, inc=1, device_id=dev, device_id_type=MESH)
    pl.semaphore_wait(barrier, len(greet))

    for copy in loads[:4]:
        copy.wait()

    def w_half(blk, n):
        return wbuf.at[blk, n // 2, :, pl.ds(n % 2 * HD, HD)]

    def w_copy(way, h, n):
        blk = lax.rem(z + NZ - h, NZ) if way == 0 else lax.rem(z + h, NZ)
        dev = {"z": zr_ if way == 0 else zl_}
        return rc(w_half(blk, n), w_half(blk, n), w_s.at[way, h, n], w_r.at[way, h, n], dev)

    def w_send(h, n):
        for way, hops in ((0, RIGHT), (1, LEFT)):
            if h < hops[n]:
                copy = w_copy(way, h, n)
                copy.start()
                sends.append(copy)

    def w_wait(h, n):
        for way, hops in ((0, RIGHT), (1, LEFT)):
            if h <= hops[n]:
                blk = lax.rem(z + NZ - h, NZ) if way == 0 else lax.rem(z + h, NZ)
                arrived(w_half(blk, n), w_s.at[way, h - 1, n], w_r.at[way, h - 1, n], {"z": zr_})

    def w_hop(h, halves):
        for n in halves:
            w_wait(h, n)
            w_send(h, n)

    early, late = (0, 1, 2), (3, 4, 5)
    for n in early:
        w_send(0, n)

    mine = pl.ds(pl.multiple_of(c * 128, 128), 128)
    there = pl.ds(pl.multiple_of(y * B + c * 128, 128), 128)
    from_y = pl.ds(pl.multiple_of(py * B + c * 128, 128), 128)
    from_c = pl.ds(pl.multiple_of(py * B + pc * 128, 128), 128)
    for j in range(NZ):
        rc(x_hbm.at[mine, cols(j, py)], xr.at[j, there, :], x_s.at[0], x_r.at[0], to_y).start()
    x_out = rc(xr.at[:, from_y, :], xr.at[:, there, :], x_s.at[0], x_r.at[0], to_y)

    for copy in loads[5:]:
        copy.wait()
    for j in range(D // B):
        gainf[j] = gain[:, j * B : (j + 1) * B].astype(F32)

    lane = lax.broadcasted_iota(jnp.int32, (B, HD), 1)
    cosb[...] = turn[0, s] * off[0] - turn[1, s] * off[1]
    sin_all = turn[1, s] * off[0] + turn[0, s] * off[1]
    sinb[...] = jnp.where(lane < HD // 2, -sin_all, sin_all)

    loads[4].wait()
    invb[own, :] = jnp.zeros((B, HD), F32)

    def squares(j, _):
        v = xin[:, pl.ds(pl.multiple_of(j * B, B), B)].astype(F32)
        invb[own, :] += v[:, :HD] * v[:, :HD] + v[:, HD:] * v[:, HD:]
        return 0

    lax.fori_loop(0, D // B, squares, 0)
    mean = jnp.sum(invb[own, :], axis=1, keepdims=True) / D
    inv_own = jnp.broadcast_to(lax.rsqrt(mean + EPS), (B, HD))
    invb[own, :] = inv_own
    isend[...] = jnp.transpose(inv_own)[:8, :]
    send(isend, irecv, i_s, i_r, to_y)

    odd = lax.rem(x, 2)
    to_n = {"x": x + 1 - 2 * odd}

    def u_rows(side, px, core):
        return xs.at[1, :, pl.ds(pl.multiple_of(side * B + px * 128 + core * 64, 64), 64), :]

    quarter = pl.ds(pl.multiple_of(odd * 128 + c * 64, 64), 64)
    row0 = pl.ds(pl.multiple_of(y * B + odd * 128 + c * 64, 64), 64)
    for j in range(NZ):
        rc(u_hbm.at[quarter, cols(j, py)], xs.at[1, j, row0, :], x_s.at[1], x_r.at[1], to_y).start()
    u_out = rc(u_rows(py, odd, c), u_rows(y, odd, c), x_s.at[1], x_r.at[1], to_y)

    def u_take(part):
        if part == 0:
            u_out.wait_recv()
            send(u_rows(py, odd, c), u_rows(py, odd, c), x_s.at[3], x_r.at[3], to_n)
            send(u_rows(py, odd, c), u_rows(py, odd, c), x_s.at[4], x_r.at[4], to_c)
        else:
            arrived(u_rows(py, 1 - odd, c), x_s.at[3], x_r.at[3], to_n)
            send(u_rows(py, 1 - odd, c), u_rows(py, 1 - odd, c), x_s.at[5], x_r.at[5], to_c)

    def u_rest():
        arrived(u_rows(py, odd, pc), x_s.at[4], x_r.at[4], to_c)
        arrived(u_rows(py, 1 - odd, pc), x_s.at[5], x_r.at[5], to_c)

    whole = pltpu.make_async_copy(xs.at[1, :, oth, :], xs.at[1, :, own, :], l_u)
    whole.wait()
    pltpu.make_async_copy(xr.at[:, oth, :], xr.at[:, own, :], l_r).wait()

    def norm_rows(rows):
        def step(j, _):
            inv = invb[rows, :]
            g = gainf[2 * j + y]
            v = xr[j, rows, :].astype(F32)
            n = jnp.concatenate([v[:, :HD] * inv, v[:, HD:] * inv], axis=1) * g
            xs[0, j, rows, :] = n.astype(BF)
            return 0

        lax.fori_loop(0, NZ, step, 0)

    norm_rows(own)

    w_hop(1, early)
    w_hop(2, early)
    x_out.wait_recv()
    send(xr.at[:, from_y, :], xr.at[:, from_y, :], x_s.at[2], x_r.at[2], to_c)
    w_hop(3, (0,))
    arrived(irecv, i_s, i_r, to_y)
    inv_oth = jnp.transpose(jnp.broadcast_to(irecv[0:1, :], (HD, B)))
    invb[oth, :] = inv_oth
    arrived(xr.at[:, from_c, :], x_s.at[2], x_r.at[2], to_c)
    norm_rows(oth)
    w_hop(3, (1,))

    def project(ch, lo, hi, start=0, width=B):
        at = pl.ds(start, width)

        def step(n, _):
            blk = lax.rem(z + 5 + n, NZ)
            acc[ch, :, at] += nn(xs[1 if ch == 2 else 0, blk], wbuf[blk, ch, :, at])
            return 0

        lax.fori_loop(lo, hi, step, 0)

    def p_copy(n):
        ch = (0, 1, 1, 2, 2)[n]
        at = (pl.ds(0, B), pl.ds(0, HD), pl.ds(HD, HD), pl.ds(0, HD), pl.ds(HD, HD))[n]
        return rc(pbuf.at[ch, :, at], rbuf.at[ch, :, at], p_s.at[n], p_r.at[n], to_y)

    def project_out(n):
        ch = (0, 1, 1, 2, 2)[n]
        at = (pl.ds(0, B), pl.ds(0, HD), pl.ds(HD, HD), pl.ds(0, HD), pl.ds(HD, HD))[n]
        pbuf[ch, :, at] = acc[ch, oth, at].astype(BF)
        p_copy(n).start()
        sends.append(p_copy(n))

    def total(n):
        p_copy(n).wait_recv()
        ch = (0, 1, 1, 2, 2)[n]
        at = (pl.ds(0, B), pl.ds(0, HD), pl.ds(HD, HD), pl.ds(0, HD), pl.ds(HD, HD))[n]
        return acc[ch, own, at] + rbuf[ch, :, at].astype(F32)

    def rot(v, sign):
        return v * cosb[...] + pltpu.roll(v, HD // 2, 1) * (sign * sinb[...])

    acc[...] = jnp.zeros_like(acc)
    project(0, 1, 6)
    w_hop(3, (2,))
    for n in late:
        w_send(0, n)
    project(0, 0, 1)
    project(0, 6, 7)
    for n in early:
        w_wait(4, n)
    project(0, 7, 8)
    project_out(0)
    project(1, 0, 8, 0, HD)
    project_out(1)
    w_hop(1, late)
    u_take(0)
    both = total(0)
    kv[0, 0] = rot(both[:, :HD], 1.0).astype(BF)
    kv[0, 1] = both[:, HD:].astype(BF)

    def kz_send(i, k):
        send(kv.at[2 * i, k], kv.at[2 * i + 2, k], kz_s.at[i, k], kv_r.at[2 * i + 2, k], {"z": zr_})

    def ky_copy(i, k):
        return rc(kv.at[2 * i + 2 * y, k], kv.at[2 * i + 1, k], ky_s.at[i, k], kv_r.at[2 * i + 1, k], to_y)

    def ky_start(i, k, side):
        @pl.when(y == side)
        def _():
            ky_copy(i, k).start()

    for k in range(2):
        kz_send(0, k)
        ky_start(0, k, 0)

    def halo(i):
        for k in range(2):
            arrived(kv.at[2 * i + 2, k], kz_s.at[i, k], kv_r.at[2 * i + 2, k], {"z": zr_})
            if i < 3:
                kz_send(i + 1, k)
                ky_start(i + 1, k, 0)
            ky_start(i, k, 1)

    def halo_odd(i):
        for k in range(2):
            arrived(kv.at[2 * i + 1, k], ky_s.at[i, k], kv_r.at[2 * i + 1, k], to_y)
            sends.append(ky_copy(i, k))

    drain()
    w_hop(2, (3,))
    halo(0)
    w_hop(2, (4, 5))
    w_hop(3, (3,))
    halo(1)
    drain()
    w_hop(3, (4, 5))
    u_take(1)
    project(1, 0, 7, HD, HD)
    u_rest()
    halo(2)
    w_wait(4, 3)
    project(1, 7, 8, HD, HD)
    project_out(2)
    project(2, 0, 7)
    w_wait(4, 4)
    project(2, 7, 8, 0, HD)
    project_out(3)
    w_wait(4, 5)
    project(2, 7, 8, HD, HD)
    project_out(4)
    drain()
    halo(3)

    for h in range(2):
        mb[h] = jnp.full((B, HD), -3e38, F32)
        lb[h] = jnp.zeros((B, HD), F32)
        oacc[h] = jnp.zeros((B, HD), F32)
        dqa[h] = jnp.zeros((B, HD), F32)
    for h in range(2):
        q = rot(total(1 + h), 1.0)
        qb[h] = q.astype(BF)
        qt[h] = jnp.transpose(q).astype(BF)

    diff = lax.broadcasted_iota(jnp.int32, (B, B), 1) - lax.broadcasted_iota(jnp.int32, (B, B), 0)

    def attend(group):
        slots = [3 * group + j for j in range(3)]
        for h in range(2):
            before = mb[h]
            scores = []
            peak = None
            for d in slots:
                top = jnp.where(s >= d, d * B, -2 * WINDOW)
                allowed = (diff <= top) & (diff > d * B - WINDOW)
                sc = jnp.where(allowed, nt(qb[h], kv[d, 0]) * SCALE, -1e30)
                sb[h, d] = sc
                both = jnp.maximum(sc[:, :HD], sc[:, HD:])
                peak = both if peak is None else jnp.maximum(peak, both)
            now = jnp.maximum(before, jnp.max(peak, axis=1, keepdims=True))
            keep = jnp.exp(before - now)
            mb[h] = now
            msl[h, group] = now
            total_l = lb[h] * keep
            total_o = oacc[h] * keep
            for d in slots:
                e = jnp.exp(sb[h, d] - jnp.concatenate([now, now], axis=1))
                sb[h, d] = e
                total_l = total_l + e[:, :HD] + e[:, HD:]
                total_o = total_o + nn(e.astype(BF), kv[d, 1])
            lb[h] = total_l
            oacc[h] = total_o

    halo_odd(0)
    attend(0)
    halo_odd(1)
    halo_odd(2)
    attend(1)
    halo_odd(3)
    attend(2)
    for h in range(2):
        v = total(3 + h)
        dob[h] = v.astype(BF)
        dot_[h] = jnp.transpose(v).astype(BF)

    for h in range(2):
        scale = jnp.broadcast_to(1.0 / jnp.sum(lb[h], axis=1, keepdims=True), (B, HD))
        lb[h] = scale
        att = (oacc[h] * scale).astype(BF)
        dl[2, own, pl.ds(h * HD, HD)] = att
        delta[h] = jnp.broadcast_to(
            jnp.sum(att.astype(F32) * dob[h].astype(F32), axis=1, keepdims=True), (B, HD)
        )

    def dl_send(ch):
        send(dl.at[ch, own, :], dl.at[ch, own, :], d_s.at[ch], d_r.at[ch], to_y)

    def slot_grads(d):
        dkt = jnp.zeros((HD, B), F32)
        dvt = jnp.zeros((HD, B), F32)
        for h in range(2):
            f = jnp.exp(msl[h, d // 3] - mb[h]) * lb[h]
            p = sb[h, d] * jnp.concatenate([f, f], axis=1)
            r = delta[h]
            ds = (p * (nt(dob[h], kv[d, 1]) - jnp.concatenate([r, r], axis=1)) * SCALE).astype(BF)
            dqa[h] += nn(ds, kv[d, 0])
            dkt = dkt + nn(qt[h], ds)
            dvt = dvt + nn(dot_[h], p.astype(BF))
        return dkt, dvt

    def piece(ref, p):
        return ref.at[p // 2, pl.ds(p % 2 * 64, 64), :]

    def y_copy(i, p):
        return rc(piece(ysrc.at[i], p), piece(yrcv.at[i], p), yr_s.at[i, p], yr_r.at[i, p], to_y)

    def slot_pair(i):
        for k, part in enumerate(slot_grads(2 * i + 1)):
            ysrc[i, k] = part.astype(BF)
        for p in range(4):
            y_copy(i, p).start()
            sends.append(y_copy(i, p))
        for k, part in enumerate(slot_grads(2 * i + 2)):
            dkve[i + 1, k] = part

    def from_partner(e, p):
        i = e // 2 - y
        keep = jnp.where((i >= 0) & (i < 4), 1.0, 0.0)
        return yrcv[jnp.clip(i, 0, 3), p // 2, pl.ds(p % 2 * 64, 64), :].astype(F32) * keep

    def chain_sum(i, p):
        e = 8 - 2 * i
        if i < 4:
            y_copy(3 - i, p).wait_recv()
        rows = pl.ds(p % 2 * 64, 64)
        part = dkve[e // 2, p // 2, rows, :] + from_partner(e, p)
        if i > 0:
            arrived(piece(zrcv.at[i - 1], p), zr_s.at[i - 1, p], zr_r.at[i - 1, p], {"z": zl_})
            part = part + zrcv[i - 1, p // 2, rows, :].astype(F32)
        return part

    def chain(i):
        for p in range(4):
            zsrc[i, p // 2, pl.ds(p % 2 * 64, 64), :] = chain_sum(i, p).astype(BF)
            send(piece(zsrc.at[i], p), piece(zrcv.at[i], p), zr_s.at[i, p], zr_r.at[i, p], {"z": zl_})

    def dlt_make(ch):
        dlt[ch] = jnp.transpose(dl[ch].astype(F32)).astype(BF)

    hops = ((3, 4, 4), (4, 3, 3))

    def g_copy(way, j, ch):
        dev = {"z": zr_ if way == 0 else zl_}
        return rc(gs.at[way, j, ch], gr.at[way, j, ch], g_s.at[way, j, ch], g_r.at[way, j, ch], dev)

    def weight_part(blk, ch):
        return nn(dlt[ch], xs[1 if ch == 2 else 0, blk])

    def g(way, j, ch):
        left = hops[way][ch] - j
        step = left if way == 0 else NZ - left
        part = weight_part(lax.rem(z + step, NZ), ch)
        if j > 0:
            g_copy(way, j - 1, ch).wait_recv()
            part = part + gr[way, j - 1, ch].astype(F32)
        gs[way, j, ch] = part.astype(BF)
        copy = g_copy(way, j, ch)
        copy.start()
        sends.append(copy)

    def query_parts(rows):
        def step(b, _):
            npart[b, rows, :] = nt(dl[1, rows, :], wbuf[b, 1])
            return 0

        lax.fori_loop(0, NZ, step, 0)

    slot_pair(3)
    slot_pair(2)
    slot_pair(1)
    slot_pair(0)
    for k, part in enumerate(slot_grads(0)):
        dkve[0, k] = part
    for h in range(2):
        dl[1, own, pl.ds(h * HD, HD)] = rot(dqa[h], -1.0).astype(BF)
    dl_send(2)
    dl_send(1)
    drain()
    chain(0)
    query_parts(own)
    x_out.wait_send()
    u_out.wait_send()
    chain(1)
    chain(2)
    chain(3)
    arrived(dl.at[2, oth, :], d_s.at[2], d_r.at[2], to_y)
    dlt_make(2)
    g(0, 0, 2)

    for p in range(4):
        dkve[0, p // 2, pl.ds(p % 2 * 64, 64), :] = chain_sum(4, p)
    dk = jnp.transpose(dkve[0, 0])
    dv = jnp.transpose(dkve[0, 1])
    dl[0, own, pl.ds(0, HD)] = rot(dk, -1.0).astype(BF)
    dl[0, own, pl.ds(HD, HD)] = dv.astype(BF)
    dl_send(0)

    rd = dk * kv[0, 0].astype(F32) + dv * kv[0, 1].astype(F32)
    for h in range(2):
        rd = rd + dqa[h] * qb[h].astype(F32)
    rd = jnp.broadcast_to(jnp.sum(rd, axis=1, keepdims=True), (B, HD))
    rds[0] = jnp.transpose(rd)[:8, :]
    send(rds.at[0], rdr, rd_s.at[0], rd_r.at[0], to_c)

    def c_copy(k, i, rows):
        return rc(cs.at[i, rows, :], cr.at[i, rows, :], c_s.at[k, i], c_r.at[k, i], to_c)

    def parts(k, rows):
        def out(i, _):
            b = 2 * i + pc
            cs[i, rows, :] = (npart[b, rows, :] + nt(dl[0, rows, :], wbuf[b, 0])).astype(BF)
            c_copy(k, i, rows).start()
            return 0

        def keep(i, _):
            b = 2 * i + c
            npart[b, rows, :] += nt(dl[0, rows, :], wbuf[b, 0])
            return 0

        lax.fori_loop(0, NX, out, 0)
        lax.fori_loop(0, NX, keep, 0)
        for i in range(NX):
            sends.append(c_copy(k, i, rows))

    def pair_sum(k, rows):
        for i in range(NX):
            c_copy(k, i, rows).wait_recv()

        def add(i, _):
            npart[2 * i + c, rows, :] += cr[i, rows, :].astype(F32)
            return 0

        lax.fori_loop(0, NX, add, 0)

    def half_rows(side, q):
        return pl.ds(pl.multiple_of(side * B + q * HD, HD), HD)

    def r_copy(way, k, q):
        dev = {"x": xp} if way == 0 else {"x": xm}
        rows = pl.ds(q * HD, HD)
        return rc(rss.at[way, k, rows, :], rsr.at[way, k, rows, :], n_s.at[way, k, q], n_r.at[way, k, q], dev)

    def r_send(way, k, blk, side, add=None):
        for q in range(2):
            part = npart[2 * blk + c, half_rows(side, q), :]
            if add is not None:
                r_copy(way, add, q).wait_recv()
                part = part + rsr[way, add, pl.ds(q * HD, HD), :].astype(F32)
            rss[way, k, pl.ds(q * HD, HD), :] = part.astype(BF)
            copy = r_copy(way, k, q)
            copy.start()
            sends.append(copy)

    parts(0, own)
    pair_sum(0, own)
    r_send(0, 0, xa, y)
    r_send(1, 0, xm, y)
    arrived(rdr, rd_s.at[0], rd_r.at[0], to_c)
    rds[1] = rds[0] + rdr[...]
    for k, dev in enumerate(({"x": xp}, {"x": xm}, {"x": xa})):
        send(rds.at[1], rdx.at[k], rd_s.at[1 + k], rd_r.at[1 + k], dev)
    arrived(dl.at[1, oth, :], d_s.at[1], d_r.at[1], to_y)
    dlt_make(1)
    g(0, 0, 1)
    g(1, 0, 2)
    g(1, 0, 1)
    g(0, 1, 2)
    drain()

    query_parts(oth)
    arrived(dl.at[0, oth, :], d_s.at[0], d_r.at[0], to_y)
    parts(1, oth)
    pair_sum(1, oth)
    r_send(1, 1, xa, py)
    r_send(0, 1, xp, y, 0)

    dlt_make(0)
    g(1, 0, 0)
    g(0, 0, 0)
    g(0, 1, 1)
    r_send(0, 2, xp, py)
    for k in range(3):
        arrived(rdx.at[k], rd_s.at[1 + k], rd_r.at[1 + k], {"x": xp})
    rds[2] = rds[1] + rdx[0] + rdx[1] + rdx[2]
    send(rds.at[2], rdy, rd_s.at[4], rd_r.at[4], to_y)
    rdb[own, :] = jnp.transpose(jnp.broadcast_to(rds[2, 0:1, :], (HD, B)))
    g(1, 1, 2)
    r_send(1, 2, xm, py, 1)

    def share(side, first, second, target, k):
        for q in range(2):
            rows, at = half_rows(side, q), pl.ds(q * HD, HD)
            r_copy(*first, q).wait_recv()
            r_copy(*second, q).wait_recv()
            n_all = npart[t, rows, :] + rsr[first[0], first[1], at, :].astype(F32)
            n_all = n_all + rsr[second[0], second[1], at, :].astype(F32)
            nd[rows, :] = n_all
            for hf in range(2):
                cut = pl.ds(hf * HD, HD)
                inv = invb[rows, :]
                v = xr[t, rows, cut].astype(F32)
                n = n_all[:, hf * HD : (hf + 1) * HD]
                gn = gainf[2 * t + y, :, cut]
                out = xs[1, t, rows, cut].astype(F32) + inv * gn * n - v * (inv * inv) * rdb[rows, :] * (1.0 / D)
                ps[rows, cut] = out.astype(BF)
            send(ps.at[rows, :], target.at[at, :], ps_s.at[k, q], ps_r.at[k, q], across)

    def gain_term(rows, cut):
        return jnp.sum(nd[rows, cut] * xr[t, rows, cut].astype(F32) * invb[rows, :], axis=0, keepdims=True)

    across = {"section": psec, "y": py}
    share(y, (0, 1), (1, 0), rel, 0)
    g(1, 1, 0)
    g(0, 1, 0)
    g(0, 2, 2)
    g(1, 1, 1)
    arrived(rdy, rd_s.at[4], rd_r.at[4], to_y)
    rdb[oth, :] = jnp.transpose(jnp.broadcast_to(rdy[0:1, :], (HD, B)))
    share(py, (0, 2), (1, 2), og.at[t, y], 1)
    for hf in range(2):
        cut = pl.ds(hf * HD, HD)
        gb[z, :, cut] = jnp.broadcast_to(gain_term(own, cut) + gain_term(oth, cut), (8, HD))

    def gb_send(h):
        blk = lax.rem(z + NZ - h, NZ)
        send(gb.at[blk], gb.at[blk], gb_s.at[0, h], gb_r.at[0, h], {"z": zr_})
        if h < 3:
            blk = lax.rem(z + h, NZ)
            send(gb.at[blk], gb.at[blk], gb_s.at[1, h], gb_r.at[1, h], {"z": zl_})

    def gb_wait(h):
        blk = lax.rem(z + NZ - h, NZ)
        arrived(gb.at[blk], gb_s.at[0, h - 1], gb_r.at[0, h - 1], {"z": zr_})
        if h < 4:
            blk = lax.rem(z + h, NZ)
            arrived(gb.at[blk], gb_s.at[1, h - 1], gb_r.at[1, h - 1], {"z": zl_})

    gb_send(0)
    g(1, 2, 0)
    g(0, 2, 1)
    drain()

    for q in range(2):
        at = pl.ds(q * HD, HD)
        arrived(rel.at[at, :], ps_s.at[0, q], ps_r.at[0, q], across)
        send(rel.at[at, :], og.at[t, py, at, :], ps_s.at[2, q], ps_r.at[2, q], to_y)

    def finish_grad(ch):
        part = weight_part(z, ch)
        for way in range(2):
            last = hops[way][ch] - 1
            g_copy(way, last, ch).wait_recv()
            part = part + gr[way, last, ch].astype(F32)
        part = jnp.transpose(part).astype(BF)
        if ch == 2:
            go[...] = part
        elif ch == 1:
            gq[...] = part
        else:
            gk[...] = part[:, :HD]
            gv[...] = part[:, HD:]

    tr, tl, ta = 2 * xm + c, 2 * xp + c, 2 * xa + c

    def og_half(blk, par, q):
        return og.at[blk, par, pl.ds(q * HD, HD), :]

    def og_send(blk, par, q, k, dev):
        send(og_half(blk, par, q), og_half(blk, par, q), og_s.at[k, q], og_r.at[k, q], dev)

    def og_wait(blk, par, q, k):
        arrived(og_half(blk, par, q), og_s.at[k, q], og_r.at[k, q], to_c)

    g(0, 2, 0)
    for q in range(2):
        arrived(og_half(t, py, q), ps_s.at[1, q], ps_r.at[1, q], across)
        og_send(t, py, q, 0, {"x": xp})
        og_send(t, py, q, 1, {"x": xm})
        og_send(t, py, q, 6, to_c)
    for q in range(2):
        arrived(og_half(t, y, q), ps_s.at[2, q], ps_r.at[2, q], to_y)
        og_send(t, y, q, 2, {"x": xp})
        og_send(t, y, q, 3, {"x": xm})
        og_send(t, y, q, 7, to_c)
    g(1, 3, 0)
    gb_wait(1)
    gb_send(1)
    g(0, 3, 2)
    g(1, 2, 2)
    for q in range(2):
        og_wait(tr, py, q, 0)
        og_send(tr, py, q, 4, {"x": xp})
        og_send(tr, py, q, 8, to_c)
    gb_wait(2)
    gb_send(2)
    g(1, 2, 1)
    g(0, 3, 1)
    for q in range(2):
        og_wait(tl, py, q, 1)
        og_send(tl, py, q, 9, to_c)
    for q in range(2):
        og_wait(tl, y, q, 3)
        og_send(tl, y, q, 5, {"x": xm})
        og_send(tl, y, q, 11, to_c)
    for q in range(2):
        og_wait(tr, y, q, 2)
        og_send(tr, y, q, 10, to_c)
    gb_wait(3)
    gb_send(3)
    drain()
    finish_grad(2)
    finish_grad(1)
    for q in range(2):
        og_wait(ta, py, q, 4)
        og_send(ta, py, q, 12, to_c)
    for q in range(2):
        og_wait(ta, y, q, 5)
        og_send(ta, y, q, 13, to_c)
    gb_wait(4)
    gsum = gb[0]
    for i in range(1, NZ):
        gsum = gsum + gb[i]
    gg[y] = gsum
    send(gg.at[y], gg.at[y], gy_s, gy_r, to_y)
    finish_grad(0)
    drain()

    sib = 1 - 2 * c
    for blk, ks in ((t, (6, 7)), (tr, (8, 10)), (tl, (9, 11)), (ta, (12, 13))):
        for q in range(2):
            og_wait(blk + sib, py, q, ks[0])
            og_wait(blk + sib, y, q, ks[1])
    arrived(gg.at[py], gy_s, gy_r, to_y)
    drain()
    drain()


def finish(og, gq, gk, gv, go, gg, passed, oq, ok, ov, oo, gain_sum, row, sems):
    copies = []
    for blk in range(8):
        for par in range(2):
            at = 2 * blk + par
            copies.append((og.at[blk, par], passed.at[0, :, pl.ds(at * B, B)]))
    copies += [(gq, oq.at[0]), (gk, ok.at[0]), (gv, ov.at[0]), (go, oo.at[0])]
    row[:, :B] = gg[0, 0:1, :]
    row[:, B:] = gg[1, 0:1, :]
    copies.append((row, gain_sum))
    started = [pltpu.make_async_copy(a, b, sems.at[i]) for i, (a, b) in enumerate(copies)]
    for copy in started:
        copy.start()
    for copy in started:
        copy.wait()


def tables():
    freq = 10000.0 ** (-2.0 * np.arange(HD // 2) / HD)
    freq = np.concatenate([freq, freq])
    off = np.arange(B)[:, None] * freq[None, :]
    blk = (np.arange(16) * B)[:, None, None] * freq[None, None, :]
    return [np.stack([np.cos(a), np.sin(a)]).astype(np.float32) for a in (off, blk)]


def per_device(layer_input, upstream, norm_gain, query_weight, key_weight, value_weight, output_weight):
    dma = pltpu.SemaphoreType.DMA
    vm = pltpu.VMEM
    scratch = [
        vm((1, D), BF), vm((2, B, HD), F32), vm((2, 16, 1, HD), F32),
        vm((D // B, 1, B), F32), vm((B, B), BF),
        vm((NZ, 3, B, B), BF), vm((2, NZ, 2 * B, B), BF), vm((NZ, 2 * B, B), BF), vm((B, D), BF),
        vm((2 * B, HD), F32), vm((8, B), F32), vm((8, B), F32), vm((3, 2 * B, B), F32),
        vm((3, B, B), BF), vm((3, B, B), BF), vm((B, HD), F32), vm((B, HD), F32),
        vm((2, B, HD), BF), vm((9, 2, B, HD), BF), vm((2, B, HD), BF), vm((2, HD, B), BF), vm((2, HD, B), BF),
        vm((2, 9, B, B), F32), vm((2, 3, B, HD), F32),
        vm((2, B, HD), F32), vm((2, B, HD), F32), vm((2, B, HD), F32), vm((2, B, HD), F32), vm((2, B, HD), F32),
        vm((5, 2, HD, B), F32), vm((4, 2, HD, B), BF), vm((4, 2, HD, B), BF), vm((4, 2, HD, B), BF), vm((4, 2, HD, B), BF),
        vm((3, 2 * B, B), BF), vm((3, B, 2 * B), BF),
        vm((3, 8, B), F32), vm((8, B), F32), vm((3, 8, B), F32), vm((8, B), F32), vm((2 * B, HD), F32),
        vm((2, 4, 3, B, B), BF), vm((2, 4, 3, B, B), BF),
        vm((NZ, 2 * B, B), F32), vm((NX, 2 * B, B), BF), vm((NX, 2 * B, B), BF),
        vm((2, 3, B, B), BF), vm((2, 3, B, B), BF), vm((2 * B, B), F32), vm((2 * B, B), BF),
        vm((NZ, 8, B), F32),
        dma((7,)), dma, dma, dma,
        dma((2, 4, 6)), dma((2, 4, 6)), dma((6,)), dma((6,)), dma, dma, dma((5,)), dma((5,)),
        dma((4, 2)), dma((4, 2)), dma((9, 2)), dma((4, 4)), dma((4, 4)), dma((4, 4)), dma((4, 4)), dma((3,)), dma((3,)),
        dma((5,)), dma((5,)), dma((2, 4, 3)), dma((2, 4, 3)), dma((2, 4)), dma((2, 4)), dma((2, 3, 2)), dma((2, 3, 2)),
        dma((3, 2)), dma((3, 2)),
        dma((14, 2)), dma((14, 2)), dma((2, 4)), dma((2, 4)), dma, dma,
    ]
    hbm = pl.BlockSpec(memory_space=pl.ANY)
    vmem = pl.BlockSpec(memory_space=pltpu.VMEM)
    og, gq, gk, gv, go, gg = pl.pallas_call(
        kernel,
        out_shape=[
            jax.ShapeDtypeStruct((8, 2, B, B), BF),
            jax.ShapeDtypeStruct((B, B), BF),
            jax.ShapeDtypeStruct((B, HD), BF),
            jax.ShapeDtypeStruct((B, HD), BF),
            jax.ShapeDtypeStruct((B, B), BF),
            jax.ShapeDtypeStruct((2, 8, B), F32),
        ],
        in_specs=[pl.BlockSpec(memory_space=pltpu.HBM)] * 9,
        out_specs=[vmem] * 6,
        scratch_shapes=scratch,
        compiler_params=pltpu.CompilerParams(
            collective_id=0, has_side_effects=True, vmem_limit_bytes=46 * 1024 * 1024
        ),
        name="step",
    )(
        *[pltpu.with_memory_space_constraint(jnp.asarray(a), pltpu.HBM) for a in (layer_input[0], upstream[0], query_weight[0], key_weight[0], value_weight[0], output_weight[0], norm_gain, *tables())],
    )
    return pl.pallas_call(
        finish,
        out_shape=[
            jax.ShapeDtypeStruct((1, B, D), BF),
            jax.ShapeDtypeStruct((1, B, B), BF),
            jax.ShapeDtypeStruct((1, B, HD), BF),
            jax.ShapeDtypeStruct((1, B, HD), BF),
            jax.ShapeDtypeStruct((1, B, B), BF),
            jax.ShapeDtypeStruct((1, 2 * B), F32),
        ],
        in_specs=[vmem] * 6,
        out_specs=[hbm] * 6,
        scratch_shapes=[vm((1, 2 * B), F32), dma((21,))],
        compiler_params=pltpu.CompilerParams(vmem_limit_bytes=8 * 1024 * 1024),
        name="finish",
    )(og, gq, gk, gv, go, gg)


def solution(mesh):
    split = Mesh(mesh.devices.reshape(2, NZ, 2, NX, 2), AXES)
    seq, tp = ("z", "y"), ("x", "c")
    rows = P("section", seq, None)
    weight = P("section", seq, tp)
    return jax.shard_map(
        per_device,
        mesh=split,
        in_specs=(rows, rows, P("section", None), weight, weight, weight, weight),
        out_specs=(rows, weight, weight, weight, weight, P("section", tp)),
        check_vma=False,
    )
```

```python
import math

import jax
import jax.numpy as jnp
import numpy as np
from jax import lax
from jax.experimental import pallas as pl
from jax.experimental.pallas import tpu as pltpu
from jax.sharding import Mesh
from jax.sharding import PartitionSpec as P

AXES = ("section", "z", "y", "x", "c")
MESH = pl.DeviceIdType.MESH
D = 4096
HD = 128
WINDOW = 2048
B = 256
NZ = 8
NX = 4
EPS = 1e-05
SCALE = 1.0 / math.sqrt(HD)
F32 = jnp.float32
BF = jnp.bfloat16
RIGHT = (4, 3, 4, 2, 2, 2)
LEFT = (3, 4, 3, 5, 5, 5)


def nt(a, b):
    return lax.dot_general(a, b, (((1,), (1,)), ((), ())), preferred_element_type=F32)


def nn(a, b):
    return lax.dot_general(a, b, (((1,), (0,)), ((), ())), preferred_element_type=F32)


def kernel(
    x_hbm, u_hbm, qw, kw, vw, ow, gain_hbm, off_hbm, blk_hbm,
    og, gq, gk, gv, go, gg,
    gain, off, turn, gainf, rel, wbuf, xs, xr, xin, invb, isend, irecv, acc, pbuf, rbuf, cosb, sinb,
    qb, kv, dob, qt, dot_, sb, msl, mb, lb, oacc, dqa, delta,
    dkve, ysrc, yrcv, zsrc, zrcv, dl, dlt, rds, rdr, rdx, rdy, rdb,
    gs, gr, npart, cs, cr, rss, rsr, nd, ps, gb,
    l_w, l_x, l_u, l_r,
    w_s, w_r, x_s, x_r, i_s, i_r, p_s, p_r,
    kz_s, ky_s, kv_r, yr_s, yr_r, zr_s, zr_r, d_s, d_r,
    rd_s, rd_r, g_s, g_r, c_s, c_r, n_s, n_r, ps_s, ps_r,
    og_s, og_r, gb_s, gb_r, gy_s, gy_r,
):
    sec = lax.axis_index("section")
    z = lax.axis_index("z")
    y = lax.axis_index("y")
    x = lax.axis_index("x")
    c = lax.axis_index("c")
    s = 2 * z + y
    t = 2 * x + c
    zr_, zl_ = lax.rem(z + 1, NZ), lax.rem(z + NZ - 1, NZ)
    xp, xm, xa = lax.rem(x + 1, NX), lax.rem(x + NX - 1, NX), lax.rem(x + 2, NX)
    py, pc, psec = 1 - y, 1 - c, 1 - sec
    to_y = {"y": py}
    to_c = {"c": pc}
    own = pl.ds(pl.multiple_of(y * B, B), B)
    oth = pl.ds(pl.multiple_of(py * B, B), B)

    def rc(src, dst, ss, rs, dev):
        return pltpu.make_async_remote_copy(
            src_ref=src, dst_ref=dst, send_sem=ss, recv_sem=rs,
            device_id=dev, device_id_type=MESH,
        )

    sends = []
    marks = [0, 0]

    def drain():
        for copy in sends[marks[0] : marks[1]]:
            copy.wait_send()
        marks[:] = [marks[1], len(sends)]

    def send(src, dst, ss, rs, dev):
        copy = rc(src, dst, ss, rs, dev)
        copy.start()
        sends.append(copy)
        return copy

    def arrived(dst, ss, rs, dev):
        rc(dst, dst, ss, rs, dev).wait_recv()

    loads = [
        pltpu.make_async_copy(kw, wbuf.at[z, 0, :, pl.ds(0, HD)], l_w.at[0]),
        pltpu.make_async_copy(vw, wbuf.at[z, 0, :, pl.ds(HD, HD)], l_w.at[1]),
        pltpu.make_async_copy(qw, wbuf.at[z, 1], l_w.at[2]),
        pltpu.make_async_copy(ow, wbuf.at[z, 2], l_w.at[3]),
        pltpu.make_async_copy(x_hbm, xin, l_x),
        pltpu.make_async_copy(gain_hbm, gain, l_w.at[4]),
        pltpu.make_async_copy(off_hbm, off, l_w.at[5]),
        pltpu.make_async_copy(blk_hbm, turn, l_w.at[6]),
    ]
    for copy in loads:
        copy.start()

    def cols(blk, parity):
        return pl.ds(pl.multiple_of((2 * blk + parity) * B, B), B)

    for j in range(NZ):
        pltpu.make_async_copy(u_hbm.at[:, cols(j, y)], xs.at[1, j, own, :], l_u).start()
        pltpu.make_async_copy(x_hbm.at[:, cols(j, y)], xr.at[j, own, :], l_r).start()

    barrier = pltpu.get_barrier_semaphore()
    greet = [
        *[{"z": lax.rem(z + k, NZ)} for k in range(1, NZ)], to_y, to_c, {"x": xp}, {"x": xm}, {"x": xa},
        {"section": psec, "y": py},
    ]
    for dev in greet:
        pl.semaphore_signal(barrier, inc=1, device_id=dev, device_id_type=MESH)
    pl.semaphore_wait(barrier, len(greet))

    for copy in loads[:4]:
        copy.wait()

    def w_half(blk, n):
        return wbuf.at[blk, n // 2, :, pl.ds(n % 2 * HD, HD)]

    def w_copy(way, h, n):
        blk = lax.rem(z + NZ - h, NZ) if way == 0 else lax.rem(z + h, NZ)
        dev = {"z": zr_ if way == 0 else zl_}
        return rc(w_half(blk, n), w_half(blk, n), w_s.at[way, h, n], w_r.at[way, h, n], dev)

    def w_send(h, n):
        for way, hops in ((0, RIGHT), (1, LEFT)):
            if h < hops[n]:
                copy = w_copy(way, h, n)
                copy.start()
                sends.append(copy)

    def w_wait(h, n):
        for way, hops in ((0, RIGHT), (1, LEFT)):
            if h <= hops[n]:
                blk = lax.rem(z + NZ - h, NZ) if way == 0 else lax.rem(z + h, NZ)
                arrived(w_half(blk, n), w_s.at[way, h - 1, n], w_r.at[way, h - 1, n], {"z": zr_})

    def w_hop(h, halves):
        for n in halves:
            w_wait(h, n)
            w_send(h, n)

    early, late = (0, 1, 2), (3, 4, 5)
    for n in early:
        w_send(0, n)

    mine = pl.ds(pl.multiple_of(c * 128, 128), 128)
    there = pl.ds(pl.multiple_of(y * B + c * 128, 128), 128)
    from_y = pl.ds(pl.multiple_of(py * B + c * 128, 128), 128)
    from_c = pl.ds(pl.multiple_of(py * B + pc * 128, 128), 128)
    for j in range(NZ):
        rc(x_hbm.at[mine, cols(j, py)], xr.at[j, there, :], x_s.at[0], x_r.at[0], to_y).start()
    x_out = rc(xr.at[:, from_y, :], xr.at[:, there, :], x_s.at[0], x_r.at[0], to_y)

    for copy in loads[5:]:
        copy.wait()
    for j in range(D // B):
        gainf[j] = gain[:, j * B : (j + 1) * B].astype(F32)

    lane = lax.broadcasted_iota(jnp.int32, (B, HD), 1)
    cosb[...] = turn[0, s] * off[0] - turn[1, s] * off[1]
    sin_all = turn[1, s] * off[0] + turn[0, s] * off[1]
    sinb[...] = jnp.where(lane < HD // 2, -sin_all, sin_all)

    loads[4].wait()
    invb[own, :] = jnp.zeros((B, HD), F32)

    def squares(j, _):
        v = xin[:, pl.ds(pl.multiple_of(j * B, B), B)].astype(F32)
        invb[own, :] += v[:, :HD] * v[:, :HD] + v[:, HD:] * v[:, HD:]
        return 0

    lax.fori_loop(0, D // B, squares, 0)
    mean = jnp.sum(invb[own, :], axis=1, keepdims=True) / D
    inv_own = jnp.broadcast_to(lax.rsqrt(mean + EPS), (B, HD))
    invb[own, :] = inv_own
    isend[...] = jnp.transpose(inv_own)[:8, :]
    send(isend, irecv, i_s, i_r, to_y)

    odd = lax.rem(x, 2)
    to_n = {"x": x + 1 - 2 * odd}

    def u_rows(side, px, core):
        return xs.at[1, :, pl.ds(pl.multiple_of(side * B + px * 128 + core * 64, 64), 64), :]

    quarter = pl.ds(pl.multiple_of(odd * 128 + c * 64, 64), 64)
    row0 = pl.ds(pl.multiple_of(y * B + odd * 128 + c * 64, 64), 64)
    for j in range(NZ):
        rc(u_hbm.at[quarter, cols(j, py)], xs.at[1, j, row0, :], x_s.at[1], x_r.at[1], to_y).start()
    u_out = rc(u_rows(py, odd, c), u_rows(y, odd, c), x_s.at[1], x_r.at[1], to_y)

    def u_take(part):
        if part == 0:
            u_out.wait_recv()
            send(u_rows(py, odd, c), u_rows(py, odd, c), x_s.at[3], x_r.at[3], to_n)
            send(u_rows(py, odd, c), u_rows(py, odd, c), x_s.at[4], x_r.at[4], to_c)
        else:
            arrived(u_rows(py, 1 - odd, c), x_s.at[3], x_r.at[3], to_n)
            send(u_rows(py, 1 - odd, c), u_rows(py, 1 - odd, c), x_s.at[5], x_r.at[5], to_c)

    def u_rest():
        arrived(u_rows(py, odd, pc), x_s.at[4], x_r.at[4], to_c)
        arrived(u_rows(py, 1 - odd, pc), x_s.at[5], x_r.at[5], to_c)

    whole = pltpu.make_async_copy(xs.at[1, :, oth, :], xs.at[1, :, own, :], l_u)
    whole.wait()
    pltpu.make_async_copy(xr.at[:, oth, :], xr.at[:, own, :], l_r).wait()

    def norm_rows(rows):
        def step(j, _):
            inv = invb[rows, :]
            g = gainf[2 * j + y]
            v = xr[j, rows, :].astype(F32)
            n = jnp.concatenate([v[:, :HD] * inv, v[:, HD:] * inv], axis=1) * g
            xs[0, j, rows, :] = n.astype(BF)
            return 0

        lax.fori_loop(0, NZ, step, 0)

    norm_rows(own)

    w_hop(1, early)
    w_hop(2, early)
    x_out.wait_recv()
    send(xr.at[:, from_y, :], xr.at[:, from_y, :], x_s.at[2], x_r.at[2], to_c)
    w_hop(3, (0,))
    arrived(irecv, i_s, i_r, to_y)
    inv_oth = jnp.transpose(jnp.broadcast_to(irecv[0:1, :], (HD, B)))
    invb[oth, :] = inv_oth
    arrived(xr.at[:, from_c, :], x_s.at[2], x_r.at[2], to_c)
    norm_rows(oth)
    w_hop(3, (1,))

    def project(ch, lo, hi, start=0, width=B):
        at = pl.ds(start, width)

        def step(n, _):
            blk = lax.rem(z + 5 + n, NZ)
            acc[ch, :, at] += nn(xs[1 if ch == 2 else 0, blk], wbuf[blk, ch, :, at])
            return 0

        lax.fori_loop(lo, hi, step, 0)

    def p_copy(n):
        ch = (0, 1, 1, 2, 2)[n]
        at = (pl.ds(0, B), pl.ds(0, HD), pl.ds(HD, HD), pl.ds(0, HD), pl.ds(HD, HD))[n]
        return rc(pbuf.at[ch, :, at], rbuf.at[ch, :, at], p_s.at[n], p_r.at[n], to_y)

    def project_out(n):
        ch = (0, 1, 1, 2, 2)[n]
        at = (pl.ds(0, B), pl.ds(0, HD), pl.ds(HD, HD), pl.ds(0, HD), pl.ds(HD, HD))[n]
        pbuf[ch, :, at] = acc[ch, oth, at].astype(BF)
        p_copy(n).start()
        sends.append(p_copy(n))

    def total(n):
        p_copy(n).wait_recv()
        ch = (0, 1, 1, 2, 2)[n]
        at = (pl.ds(0, B), pl.ds(0, HD), pl.ds(HD, HD), pl.ds(0, HD), pl.ds(HD, HD))[n]
        return acc[ch, own, at] + rbuf[ch, :, at].astype(F32)

    def rot(v, sign):
        return v * cosb[...] + pltpu.roll(v, HD // 2, 1) * (sign * sinb[...])

    acc[...] = jnp.zeros_like(acc)
    project(0, 1, 6)
    w_hop(3, (2,))
    for n in late:
        w_send(0, n)
    project(0, 0, 1)
    project(0, 6, 7)
    for n in early:
        w_wait(4, n)
    project(0, 7, 8)
    project_out(0)
    project(1, 0, 8, 0, HD)
    project_out(1)
    w_hop(1, late)
    u_take(0)
    both = total(0)
    kv[0, 0] = rot(both[:, :HD], 1.0).astype(BF)
    kv[0, 1] = both[:, HD:].astype(BF)

    def kz_send(i, k):
        send(kv.at[2 * i, k], kv.at[2 * i + 2, k], kz_s.at[i, k], kv_r.at[2 * i + 2, k], {"z": zr_})

    def ky_copy(i, k):
        return rc(kv.at[2 * i + 2 * y, k], kv.at[2 * i + 1, k], ky_s.at[i, k], kv_r.at[2 * i + 1, k], to_y)

    def ky_start(i, k, side):
        @pl.when(y == side)
        def _():
            ky_copy(i, k).start()

    for k in range(2):
        kz_send(0, k)
        ky_start(0, k, 0)

    def halo(i):
        for k in range(2):
            arrived(kv.at[2 * i + 2, k], kz_s.at[i, k], kv_r.at[2 * i + 2, k], {"z": zr_})
            if i < 3:
                kz_send(i + 1, k)
                ky_start(i + 1, k, 0)
            ky_start(i, k, 1)

    def halo_odd(i):
        for k in range(2):
            arrived(kv.at[2 * i + 1, k], ky_s.at[i, k], kv_r.at[2 * i + 1, k], to_y)
            sends.append(ky_copy(i, k))

    drain()
    w_hop(2, (3,))
    halo(0)
    w_hop(2, (4, 5))
    w_hop(3, (3,))
    halo(1)
    drain()
    w_hop(3, (4, 5))
    u_take(1)
    project(1, 1, 7, HD, HD)
    u_rest()
    w_hop(4, late)
    halo(2)
    project(2, 1, 7)
    project(1, 7, 8, HD, HD)
    w_wait(5, 3)
    project(1, 0, 1, HD, HD)
    project_out(2)
    project(2, 7, 8)
    w_wait(5, 4)
    project(2, 0, 1, 0, HD)
    project_out(3)
    w_wait(5, 5)
    project(2, 0, 1, HD, HD)
    project_out(4)
    drain()
    halo(3)

    for h in range(2):
        mb[h] = jnp.full((B, HD), -3e38, F32)
        lb[h] = jnp.zeros((B, HD), F32)
        oacc[h] = jnp.zeros((B, HD), F32)
        dqa[h] = jnp.zeros((B, HD), F32)
    for h in range(2):
        q = rot(total(1 + h), 1.0)
        qb[h] = q.astype(BF)
        qt[h] = jnp.transpose(q).astype(BF)

    diff = lax.broadcasted_iota(jnp.int32, (B, B), 1) - lax.broadcasted_iota(jnp.int32, (B, B), 0)

    def attend(group):
        slots = [3 * group + j for j in range(3)]
        for h in range(2):
            before = mb[h]
            scores = []
            peak = None
            for d in slots:
                top = jnp.where(s >= d, d * B, -2 * WINDOW)
                allowed = (diff <= top) & (diff > d * B - WINDOW)
                sc = jnp.where(allowed, nt(qb[h], kv[d, 0]) * SCALE, -1e30)
                sb[h, d] = sc
                both = jnp.maximum(sc[:, :HD], sc[:, HD:])
                peak = both if peak is None else jnp.maximum(peak, both)
            now = jnp.maximum(before, jnp.max(peak, axis=1, keepdims=True))
            keep = jnp.exp(before - now)
            mb[h] = now
            msl[h, group] = now
            total_l = lb[h] * keep
            total_o = oacc[h] * keep
            for d in slots:
                e = jnp.exp(sb[h, d] - jnp.concatenate([now, now], axis=1))
                sb[h, d] = e
                total_l = total_l + e[:, :HD] + e[:, HD:]
                total_o = total_o + nn(e.astype(BF), kv[d, 1])
            lb[h] = total_l
            oacc[h] = total_o

    halo_odd(0)
    attend(0)
    halo_odd(1)
    halo_odd(2)
    attend(1)
    halo_odd(3)
    attend(2)
    for h in range(2):
        v = total(3 + h)
        dob[h] = v.astype(BF)
        dot_[h] = jnp.transpose(v).astype(BF)

    for h in range(2):
        scale = jnp.broadcast_to(1.0 / jnp.sum(lb[h], axis=1, keepdims=True), (B, HD))
        lb[h] = scale
        att = (oacc[h] * scale).astype(BF)
        dl[2, own, pl.ds(h * HD, HD)] = att
        delta[h] = jnp.broadcast_to(
            jnp.sum(att.astype(F32) * dob[h].astype(F32), axis=1, keepdims=True), (B, HD)
        )

    def dl_send(ch):
        send(dl.at[ch, own, :], dl.at[ch, own, :], d_s.at[ch], d_r.at[ch], to_y)

    def slot_grads(d):
        dkt = jnp.zeros((HD, B), F32)
        dvt = jnp.zeros((HD, B), F32)
        for h in range(2):
            f = jnp.exp(msl[h, d // 3] - mb[h]) * lb[h]
            p = sb[h, d] * jnp.concatenate([f, f], axis=1)
            r = delta[h]
            ds = (p * (nt(dob[h], kv[d, 1]) - jnp.concatenate([r, r], axis=1)) * SCALE).astype(BF)
            dqa[h] += nn(ds, kv[d, 0])
            dkt = dkt + nn(qt[h], ds)
            dvt = dvt + nn(dot_[h], p.astype(BF))
        return dkt, dvt

    def piece(ref, p):
        return ref.at[p // 2, pl.ds(p % 2 * 64, 64), :]

    def y_copy(i, p):
        return rc(piece(ysrc.at[i], p), piece(yrcv.at[i], p), yr_s.at[i, p], yr_r.at[i, p], to_y)

    def slot_pair(i):
        for k, part in enumerate(slot_grads(2 * i + 1)):
            ysrc[i, k] = part.astype(BF)
        for p in range(4):
            y_copy(i, p).start()
            sends.append(y_copy(i, p))
        for k, part in enumerate(slot_grads(2 * i + 2)):
            dkve[i + 1, k] = part

    def from_partner(e, p):
        i = e // 2 - y
        keep = jnp.where((i >= 0) & (i < 4), 1.0, 0.0)
        return yrcv[jnp.clip(i, 0, 3), p // 2, pl.ds(p % 2 * 64, 64), :].astype(F32) * keep

    def chain_sum(i, p):
        e = 8 - 2 * i
        if i < 4:
            y_copy(3 - i, p).wait_recv()
        rows = pl.ds(p % 2 * 64, 64)
        part = dkve[e // 2, p // 2, rows, :] + from_partner(e, p)
        if i > 0:
            arrived(piece(zrcv.at[i - 1], p), zr_s.at[i - 1, p], zr_r.at[i - 1, p], {"z": zl_})
            part = part + zrcv[i - 1, p // 2, rows, :].astype(F32)
        return part

    def chain(i):
        for p in range(4):
            zsrc[i, p // 2, pl.ds(p % 2 * 64, 64), :] = chain_sum(i, p).astype(BF)
            send(piece(zsrc.at[i], p), piece(zrcv.at[i], p), zr_s.at[i, p], zr_r.at[i, p], {"z": zl_})

    def dlt_make(ch):
        dlt[ch] = jnp.transpose(dl[ch].astype(F32)).astype(BF)

    hops = ((3, 4, 4), (4, 3, 3))

    def g_copy(way, j, ch):
        dev = {"z": zr_ if way == 0 else zl_}
        return rc(gs.at[way, j, ch], gr.at[way, j, ch], g_s.at[way, j, ch], g_r.at[way, j, ch], dev)

    def weight_part(blk, ch):
        return nn(dlt[ch], xs[1 if ch == 2 else 0, blk])

    def g(way, j, ch):
        left = hops[way][ch] - j
        step = left if way == 0 else NZ - left
        part = weight_part(lax.rem(z + step, NZ), ch)
        if j > 0:
            g_copy(way, j - 1, ch).wait_recv()
            part = part + gr[way, j - 1, ch].astype(F32)
        gs[way, j, ch] = part.astype(BF)
        copy = g_copy(way, j, ch)
        copy.start()
        sends.append(copy)

    def query_parts(rows):
        def step(b, _):
            npart[b, rows, :] = nt(dl[1, rows, :], wbuf[b, 1])
            return 0

        lax.fori_loop(0, NZ, step, 0)

    slot_pair(3)
    slot_pair(2)
    slot_pair(1)
    slot_pair(0)
    for k, part in enumerate(slot_grads(0)):
        dkve[0, k] = part
    for h in range(2):
        dl[1, own, pl.ds(h * HD, HD)] = rot(dqa[h], -1.0).astype(BF)
    dl_send(2)
    dl_send(1)
    drain()
    chain(0)
    query_parts(own)
    x_out.wait_send()
    u_out.wait_send()
    chain(1)
    chain(2)
    chain(3)
    arrived(dl.at[2, oth, :], d_s.at[2], d_r.at[2], to_y)
    dlt_make(2)
    g(0, 0, 2)

    for p in range(4):
        dkve[0, p // 2, pl.ds(p % 2 * 64, 64), :] = chain_sum(4, p)
    dk = jnp.transpose(dkve[0, 0])
    dv = jnp.transpose(dkve[0, 1])
    dl[0, own, pl.ds(0, HD)] = rot(dk, -1.0).astype(BF)
    dl[0, own, pl.ds(HD, HD)] = dv.astype(BF)
    dl_send(0)

    rd = dk * kv[0, 0].astype(F32) + dv * kv[0, 1].astype(F32)
    for h in range(2):
        rd = rd + dqa[h] * qb[h].astype(F32)
    rd = jnp.broadcast_to(jnp.sum(rd, axis=1, keepdims=True), (B, HD))
    rds[0] = jnp.transpose(rd)[:8, :]
    send(rds.at[0], rdr, rd_s.at[0], rd_r.at[0], to_c)

    def c_copy(k, i, rows):
        return rc(cs.at[i, rows, :], cr.at[i, rows, :], c_s.at[k, i], c_r.at[k, i], to_c)

    def parts(k, rows):
        def out(i, _):
            b = 2 * i + pc
            cs[i, rows, :] = (npart[b, rows, :] + nt(dl[0, rows, :], wbuf[b, 0])).astype(BF)
            c_copy(k, i, rows).start()
            return 0

        def keep(i, _):
            b = 2 * i + c
            npart[b, rows, :] += nt(dl[0, rows, :], wbuf[b, 0])
            return 0

        lax.fori_loop(0, NX, out, 0)
        lax.fori_loop(0, NX, keep, 0)
        for i in range(NX):
            sends.append(c_copy(k, i, rows))

    def pair_sum(k, rows):
        for i in range(NX):
            c_copy(k, i, rows).wait_recv()

        def add(i, _):
            npart[2 * i + c, rows, :] += cr[i, rows, :].astype(F32)
            return 0

        lax.fori_loop(0, NX, add, 0)

    def half_rows(side, q):
        return pl.ds(pl.multiple_of(side * B + q * HD, HD), HD)

    def r_copy(way, k, q):
        dev = {"x": xp} if way == 0 else {"x": xm}
        rows = pl.ds(q * HD, HD)
        return rc(rss.at[way, k, rows, :], rsr.at[way, k, rows, :], n_s.at[way, k, q], n_r.at[way, k, q], dev)

    def r_send(way, k, blk, side, add=None):
        for q in range(2):
            part = npart[2 * blk + c, half_rows(side, q), :]
            if add is not None:
                r_copy(way, add, q).wait_recv()
                part = part + rsr[way, add, pl.ds(q * HD, HD), :].astype(F32)
            rss[way, k, pl.ds(q * HD, HD), :] = part.astype(BF)
            copy = r_copy(way, k, q)
            copy.start()
            sends.append(copy)

    g(1, 0, 2)
    parts(0, own)
    pair_sum(0, own)
    r_send(0, 0, xa, y)
    r_send(1, 0, xm, y)
    arrived(rdr, rd_s.at[0], rd_r.at[0], to_c)
    rds[1] = rds[0] + rdr[...]
    for k, dev in enumerate(({"x": xp}, {"x": xm}, {"x": xa})):
        send(rds.at[1], rdx.at[k], rd_s.at[1 + k], rd_r.at[1 + k], dev)
    arrived(dl.at[1, oth, :], d_s.at[1], d_r.at[1], to_y)
    dlt_make(1)
    g(0, 0, 1)
    g(1, 0, 1)
    g(0, 1, 2)
    g(1, 1, 2)
    drain()

    query_parts(oth)
    arrived(dl.at[0, oth, :], d_s.at[0], d_r.at[0], to_y)
    parts(1, oth)
    pair_sum(1, oth)
    r_send(1, 1, xa, py)
    r_send(0, 1, xp, y, 0)

    dlt_make(0)
    g(1, 0, 0)
    g(0, 0, 0)
    g(0, 1, 1)
    r_send(0, 2, xp, py)
    for k in range(3):
        arrived(rdx.at[k], rd_s.at[1 + k], rd_r.at[1 + k], {"x": xp})
    rds[2] = rds[1] + rdx[0] + rdx[1] + rdx[2]
    send(rds.at[2], rdy, rd_s.at[4], rd_r.at[4], to_y)
    rdb[own, :] = jnp.transpose(jnp.broadcast_to(rds[2, 0:1, :], (HD, B)))
    g(1, 1, 1)
    r_send(1, 2, xm, py, 1)

    def share(side, first, second, target, k):
        for q in range(2):
            rows, at = half_rows(side, q), pl.ds(q * HD, HD)
            r_copy(*first, q).wait_recv()
            r_copy(*second, q).wait_recv()
            n_all = npart[t, rows, :] + rsr[first[0], first[1], at, :].astype(F32)
            n_all = n_all + rsr[second[0], second[1], at, :].astype(F32)
            nd[rows, :] = n_all
            for hf in range(2):
                cut = pl.ds(hf * HD, HD)
                inv = invb[rows, :]
                v = xr[t, rows, cut].astype(F32)
                n = n_all[:, hf * HD : (hf + 1) * HD]
                gn = gainf[2 * t + y, :, cut]
                out = xs[1, t, rows, cut].astype(F32) + inv * gn * n - v * (inv * inv) * rdb[rows, :] * (1.0 / D)
                ps[rows, cut] = out.astype(BF)
            send(ps.at[rows, :], target.at[at, :], ps_s.at[k, q], ps_r.at[k, q], across)

    def gain_term(rows, cut):
        return jnp.sum(nd[rows, cut] * xr[t, rows, cut].astype(F32) * invb[rows, :], axis=0, keepdims=True)

    across = {"section": psec, "y": py}
    share(y, (0, 1), (1, 0), rel, 0)
    g(0, 2, 2)
    g(1, 2, 2)
    arrived(rdy, rd_s.at[4], rd_r.at[4], to_y)
    rdb[oth, :] = jnp.transpose(jnp.broadcast_to(rdy[0:1, :], (HD, B)))
    share(py, (0, 2), (1, 2), og.at[t, y], 1)
    for hf in range(2):
        cut = pl.ds(hf * HD, HD)
        gb[z, :, cut] = jnp.broadcast_to(gain_term(own, cut) + gain_term(oth, cut), (8, HD))

    for k in range(1, NZ):
        send(gb.at[z], gb.at[z], gb_s.at[k - 1], gb_r.at[k - 1], {"z": lax.rem(z + k, NZ)})

    def gain_sum():
        for k in range(1, NZ):
            arrived(gb.at[lax.rem(z + NZ - k, NZ)], gb_s.at[k - 1], gb_r.at[k - 1], {"z": zr_})
        gsum = gb[0]
        for i in range(1, NZ):
            gsum = gsum + gb[i]
        gg[y] = gsum
        send(gg.at[y], gg.at[y], gy_s, gy_r, to_y)

    g(1, 1, 0)
    g(0, 1, 0)

    for q in range(2):
        at = pl.ds(q * HD, HD)
        arrived(rel.at[at, :], ps_s.at[0, q], ps_r.at[0, q], across)
        send(rel.at[at, :], og.at[t, py, at, :], ps_s.at[2, q], ps_r.at[2, q], to_y)

    def finish_grad(ch):
        part = weight_part(z, ch)
        for way in range(2):
            last = hops[way][ch] - 1
            g_copy(way, last, ch).wait_recv()
            part = part + gr[way, last, ch].astype(F32)
        part = jnp.transpose(part).astype(BF)
        if ch == 2:
            go[...] = part
        elif ch == 1:
            gq[...] = part
        else:
            gk[...] = part[:, :HD]
            gv[...] = part[:, HD:]

    tr, tl, ta = 2 * xm + c, 2 * xp + c, 2 * xa + c

    def og_half(blk, par, q):
        return og.at[blk, par, pl.ds(q * HD, HD), :]

    def og_send(blk, par, q, k, dev):
        send(og_half(blk, par, q), og_half(blk, par, q), og_s.at[k, q], og_r.at[k, q], dev)

    def og_wait(blk, par, q, k):
        arrived(og_half(blk, par, q), og_s.at[k, q], og_r.at[k, q], to_c)

    g(0, 2, 1)
    for q in range(2):
        arrived(og_half(t, py, q), ps_s.at[1, q], ps_r.at[1, q], across)
        og_send(t, py, q, 0, {"x": xp})
        og_send(t, py, q, 1, {"x": xm})
        og_send(t, py, q, 6, to_c)
    for q in range(2):
        arrived(og_half(t, y, q), ps_s.at[2, q], ps_r.at[2, q], to_y)
        og_send(t, y, q, 2, {"x": xp})
        og_send(t, y, q, 3, {"x": xm})
        og_send(t, y, q, 7, to_c)
    g(1, 2, 0)
    g(0, 2, 0)
    g(0, 3, 2)
    for q in range(2):
        og_wait(tr, py, q, 0)
        og_send(tr, py, q, 4, {"x": xp})
        og_send(tr, py, q, 8, to_c)
    for q in range(2):
        og_wait(tl, py, q, 1)
        og_send(tl, py, q, 9, to_c)
    g(1, 2, 1)
    g(0, 3, 1)
    for q in range(2):
        og_wait(tl, y, q, 3)
        og_send(tl, y, q, 5, {"x": xm})
        og_send(tl, y, q, 11, to_c)
    for q in range(2):
        og_wait(tr, y, q, 2)
        og_send(tr, y, q, 10, to_c)
    g(1, 3, 0)
    for q in range(2):
        og_wait(ta, py, q, 4)
        og_send(ta, py, q, 12, to_c)
    for q in range(2):
        og_wait(ta, y, q, 5)
        og_send(ta, y, q, 13, to_c)
    gain_sum()
    finish_grad(2)
    finish_grad(1)
    drain()
    finish_grad(0)
    drain()

    sib = 1 - 2 * c
    for blk, ks in ((t, (6, 7)), (tr, (8, 10)), (tl, (9, 11)), (ta, (12, 13))):
        for q in range(2):
            og_wait(blk + sib, py, q, ks[0])
            og_wait(blk + sib, y, q, ks[1])
    arrived(gg.at[py], gy_s, gy_r, to_y)
    drain()
    drain()


def finish(og, gq, gk, gv, go, gg, passed, oq, ok, ov, oo, gain_sum, row, sems):
    copies = []
    for blk in range(8):
        for par in range(2):
            at = 2 * blk + par
            copies.append((og.at[blk, par], passed.at[0, :, pl.ds(at * B, B)]))
    copies += [(gq, oq.at[0]), (gk, ok.at[0]), (gv, ov.at[0]), (go, oo.at[0])]
    row[:, :B] = gg[0, 0:1, :]
    row[:, B:] = gg[1, 0:1, :]
    copies.append((row, gain_sum))
    started = [pltpu.make_async_copy(a, b, sems.at[i]) for i, (a, b) in enumerate(copies)]
    for copy in started:
        copy.start()
    for copy in started:
        copy.wait()


def tables():
    freq = 10000.0 ** (-2.0 * np.arange(HD // 2) / HD)
    freq = np.concatenate([freq, freq])
    off = np.arange(B)[:, None] * freq[None, :]
    blk = (np.arange(16) * B)[:, None, None] * freq[None, None, :]
    return [np.stack([np.cos(a), np.sin(a)]).astype(np.float32) for a in (off, blk)]


def per_device(layer_input, upstream, norm_gain, query_weight, key_weight, value_weight, output_weight):
    dma = pltpu.SemaphoreType.DMA
    vm = pltpu.VMEM
    scratch = [
        vm((1, D), BF), vm((2, B, HD), F32), vm((2, 16, 1, HD), F32),
        vm((D // B, 1, B), F32), vm((B, B), BF),
        vm((NZ, 3, B, B), BF), vm((2, NZ, 2 * B, B), BF), vm((NZ, 2 * B, B), BF), vm((B, D), BF),
        vm((2 * B, HD), F32), vm((8, B), F32), vm((8, B), F32), vm((3, 2 * B, B), F32),
        vm((3, B, B), BF), vm((3, B, B), BF), vm((B, HD), F32), vm((B, HD), F32),
        vm((2, B, HD), BF), vm((9, 2, B, HD), BF), vm((2, B, HD), BF), vm((2, HD, B), BF), vm((2, HD, B), BF),
        vm((2, 9, B, B), F32), vm((2, 3, B, HD), F32),
        vm((2, B, HD), F32), vm((2, B, HD), F32), vm((2, B, HD), F32), vm((2, B, HD), F32), vm((2, B, HD), F32),
        vm((5, 2, HD, B), F32), vm((4, 2, HD, B), BF), vm((4, 2, HD, B), BF), vm((4, 2, HD, B), BF), vm((4, 2, HD, B), BF),
        vm((3, 2 * B, B), BF), vm((3, B, 2 * B), BF),
        vm((3, 8, B), F32), vm((8, B), F32), vm((3, 8, B), F32), vm((8, B), F32), vm((2 * B, HD), F32),
        vm((2, 4, 3, B, B), BF), vm((2, 4, 3, B, B), BF),
        vm((NZ, 2 * B, B), F32), vm((NX, 2 * B, B), BF), vm((NX, 2 * B, B), BF),
        vm((2, 3, B, B), BF), vm((2, 3, B, B), BF), vm((2 * B, B), F32), vm((2 * B, B), BF),
        vm((NZ, 8, B), F32),
        dma((7,)), dma, dma, dma,
        dma((2, 5, 6)), dma((2, 5, 6)), dma((6,)), dma((6,)), dma, dma, dma((5,)), dma((5,)),
        dma((4, 2)), dma((4, 2)), dma((9, 2)), dma((4, 4)), dma((4, 4)), dma((4, 4)), dma((4, 4)), dma((3,)), dma((3,)),
        dma((5,)), dma((5,)), dma((2, 4, 3)), dma((2, 4, 3)), dma((2, 4)), dma((2, 4)), dma((2, 3, 2)), dma((2, 3, 2)),
        dma((3, 2)), dma((3, 2)),
        dma((14, 2)), dma((14, 2)), dma((7,)), dma((7,)), dma, dma,
    ]
    hbm = pl.BlockSpec(memory_space=pl.ANY)
    vmem = pl.BlockSpec(memory_space=pltpu.VMEM)
    og, gq, gk, gv, go, gg = pl.pallas_call(
        kernel,
        out_shape=[
            jax.ShapeDtypeStruct((8, 2, B, B), BF),
            jax.ShapeDtypeStruct((B, B), BF),
            jax.ShapeDtypeStruct((B, HD), BF),
            jax.ShapeDtypeStruct((B, HD), BF),
            jax.ShapeDtypeStruct((B, B), BF),
            jax.ShapeDtypeStruct((2, 8, B), F32),
        ],
        in_specs=[pl.BlockSpec(memory_space=pltpu.HBM)] * 9,
        out_specs=[vmem] * 6,
        scratch_shapes=scratch,
        compiler_params=pltpu.CompilerParams(
            collective_id=0, has_side_effects=True, vmem_limit_bytes=46 * 1024 * 1024
        ),
        name="step",
    )(
        *[pltpu.with_memory_space_constraint(jnp.asarray(a), pltpu.HBM) for a in (layer_input[0], upstream[0], query_weight[0], key_weight[0], value_weight[0], output_weight[0], norm_gain, *tables())],
    )
    return pl.pallas_call(
        finish,
        out_shape=[
            jax.ShapeDtypeStruct((1, B, D), BF),
            jax.ShapeDtypeStruct((1, B, B), BF),
            jax.ShapeDtypeStruct((1, B, HD), BF),
            jax.ShapeDtypeStruct((1, B, HD), BF),
            jax.ShapeDtypeStruct((1, B, B), BF),
            jax.ShapeDtypeStruct((1, 2 * B), F32),
        ],
        in_specs=[vmem] * 6,
        out_specs=[hbm] * 6,
        scratch_shapes=[vm((1, 2 * B), F32), dma((21,))],
        compiler_params=pltpu.CompilerParams(vmem_limit_bytes=8 * 1024 * 1024),
        name="finish",
    )(og, gq, gk, gv, go, gg)


def solution(mesh):
    split = Mesh(mesh.devices.reshape(2, NZ, 2, NX, 2), AXES)
    seq, tp = ("z", "y"), ("x", "c")
    rows = P("section", seq, None)
    weight = P("section", seq, tp)
    return jax.shard_map(
        per_device,
        mesh=split,
        in_specs=(rows, rows, P("section", None), weight, weight, weight, weight),
        out_specs=(rows, weight, weight, weight, weight, P("section", tp)),
        check_vma=False,
    )
```
